256 devices in a mesh: grp: 8 (over z_hi, x), tile: 32 (over z_lo, y, core).
Axes of the slice: x: 4, y: 4, z: 8 (z_hi: 2, z_lo: 4; z = z_hi * 4 + z_lo), core: 2. Of those that a mesh axis runs over, the one named last changes fastest.
Arguments:
- visibility: bfloat16 [2, 512, 512, 1024], P(None, 'tile', None, 'grp'), may hold values from -3 to 3, as said below
- dish_pair_okay: int32 [512, 512], P('tile'), may hold values 0 or 1
- triangles: int32 [3, 65536], P(None, 'tile'), may hold values from 0 to 511, as said below
Outputs:
- triangle_means: float32 [2, 65536], P(None, 'tile')
- closure_spectrum: float32 [2, 1024], P(None, ('grp', 'tile'))
The draws below stay inside these ranges and needn't reach their ends.
Inputs may be any that keep to these rules, and one draw needn't show every extreme that they name: Both parts of every visibility lie in -3 to 3. `triangles`: column j belongs to block d = j // 2048 and level k = (j % 2048) // 1024; its first antenna lies in block d (antennas d * 16 to d * 16 + 15), its second in block d XOR 2**k, and its third is any antenna other than the first two.
All inputs are finite; a program needn't handle non-finite values. No bound on the sum of `dish_pair_okay` on one device may be relied on, other than what follows from the above.
Results may differ from the reference program's by a relative error of at most 0.0003.
Values may be sent and summed in bfloat16 or wider, within the bound.
A program may use at most 64 MiB of HBM per device.

```python
import math
import jax
import jax.numpy as jnp
from jax import lax

RECEIVER_DISHES = 512
RADIO_BANDS = 1024
TRI_LVL = 1024
TA = 16
TRI_DEV = 2048
THREE_DISH_SETS = 65536


def draw_visibility(key, part):
    seed_sequence = jax.random.split(key, 3)
    rotation_angles = jax.random.uniform(seed_sequence[0], (RECEIVER_DISHES, RADIO_BANDS), jnp.float32, -math.pi, math.pi)
    loudness_scale = 0.8 + 0.4 * jax.random.uniform(seed_sequence[1], (RECEIVER_DISHES, RADIO_BANDS), jnp.float32)
    hiss_component = 0.3 * jnp.clip(jax.random.normal(seed_sequence[2], (2, RECEIVER_DISHES, RECEIVER_DISHES, RADIO_BANDS), jnp.float32), -4.0, 4.0)
    gain_real = loudness_scale * jnp.cos(rotation_angles)
    gain_imag = loudness_scale * jnp.sin(rotation_angles)
    signal_real = gain_real[:, None, :] * gain_real[None, :, :] + gain_imag[:, None, :] * gain_imag[None, :, :]
    signal_imag = gain_imag[:, None, :] * gain_real[None, :, :] - gain_real[:, None, :] * gain_imag[None, :, :]
    return (jnp.stack([signal_real, signal_imag]) + hiss_component).astype(jnp.bfloat16)


def draw_triangles(key, part):
    seed_sequence = jax.random.split(key, 3)
    column = jnp.arange(THREE_DISH_SETS, dtype=jnp.int32)
    block_index = column // TRI_DEV
    level_index = column % TRI_DEV // TRI_LVL
    partner = jnp.bitwise_xor(block_index, jnp.left_shift(jnp.ones_like(level_index), level_index))
    first = block_index * TA + jax.random.randint(seed_sequence[0], (THREE_DISH_SETS,), 0, TA, jnp.int32)
    second = partner * TA + jax.random.randint(seed_sequence[1], (THREE_DISH_SETS,), 0, TA, jnp.int32)
    lower = jnp.minimum(first, second)
    upper = jnp.maximum(first, second)
    vertex_point = jax.random.randint(seed_sequence[2], (THREE_DISH_SETS,), 0, RECEIVER_DISHES - 2, jnp.int32)
    vertex_point = vertex_point + (vertex_point >= lower).astype(jnp.int32)
    vertex_point = vertex_point + (vertex_point >= upper).astype(jnp.int32)
    return jnp.stack([first, second, vertex_point]).astype(jnp.int32)


def place_ends(result, own_key, low, largest):
    spot = [jax.random.randint(jax.random.fold_in(own_key, axis), (), 0, length) for axis, length in enumerate(result.shape)]
    widest = result.shape.index(max(result.shape))
    beside = spot[:widest] + [(spot[widest] + 1) % result.shape[widest]] + spot[widest + 1:]
    return result.at[tuple(spot)].set(low).at[tuple(beside)].set(largest)


def setup_inputs(seed: int = 0) -> dict:
    seeds = jax.random.split(jax.random.key(seed), 4)
    return {
        "visibility": draw_visibility(jax.random.fold_in(seeds[3], 71), 0),
        "dish_pair_okay": place_ends((jax.random.randint(seeds[1], (RECEIVER_DISHES, RECEIVER_DISHES), 0, 8) < 7).astype(jnp.int32), jax.random.fold_in(seeds[1], 1), 0, 1),
        "triangles": draw_triangles(jax.random.fold_in(seeds[3], 71), 0),
    }


def bispectrum(edge_ab, edge_bc, edge_ac):
    edge_ab = edge_ab.astype(jnp.float32)
    edge_bc = edge_bc.astype(jnp.float32)
    edge_ac = edge_ac.astype(jnp.float32)
    prod_real = edge_ab[0] * edge_bc[0] - edge_ab[1] * edge_bc[1]
    prod_imag = edge_ab[0] * edge_bc[1] + edge_ab[1] * edge_bc[0]
    real_part = prod_real * edge_ac[0] + prod_imag * edge_ac[1]
    imag_part = prod_imag * edge_ac[0] - prod_real * edge_ac[1]
    return (real_part, imag_part)

def reference(visibility, dish_pair_okay, triangles):
    flag_table = dish_pair_okay.astype(jnp.float32)
    count = triangles.shape[1] // TRI_LVL
    blocks = jnp.transpose(triangles.reshape(3, count, TRI_LVL), (1, 0, 2))

    def step(carry, block):
        first, second, vertex_point = (block[0], block[1], block[2])
        edge_ab = visibility[:, first, second, :]
        edge_bc = visibility[:, second, vertex_point, :]
        edge_ac = visibility[:, first, vertex_point, :]
        weight = flag_table[first, second] * flag_table[second, vertex_point] * flag_table[first, vertex_point]
        real_part, imag_part = bispectrum(edge_ab, edge_bc, edge_ac)
        weighted_real = weight[:, None] * real_part
        weighted_imag = weight[:, None] * imag_part
        magnitude = weight[:, None] * jnp.sqrt(real_part * real_part + imag_part * imag_part)
        new_carry = (carry[0] + lax.optimization_barrier(jnp.sum(weighted_real, 0)), carry[1] + lax.optimization_barrier(jnp.sum(weighted_imag, 0)), carry[2] + lax.optimization_barrier(jnp.sum(magnitude, 0)))
        means = jnp.stack([lax.optimization_barrier(jnp.sum(weighted_real, 1)), lax.optimization_barrier(jnp.sum(weighted_imag, 1))]) / RADIO_BANDS
        return (new_carry, means)
    start = (jnp.zeros((RADIO_BANDS,), jnp.float32), jnp.zeros((RADIO_BANDS,), jnp.float32), jnp.zeros((RADIO_BANDS,), jnp.float32))
    totals, means = lax.scan(step, start, blocks)
    triangle_means = jnp.transpose(means, (1, 0, 2)).reshape(2, count * TRI_LVL)
    closure_spectrum = jnp.stack([totals[0], totals[1]]) / (1.0 + totals[2])
    return (triangle_means, closure_spectrum)
```

```python
import jax
import jax.numpy as jnp
from jax import lax
from jax.experimental import pallas as pl
from jax.experimental.pallas import tpu as pltpu
from jax.sharding import PartitionSpec as P

RADIO_BANDS = 1024
TRI_LVL = 1024
LEVELS = 2
CHUNK = 256
CHUNKS = TRI_LVL // CHUNK
PIECES = LEVELS * CHUNKS
UNROLL = 32
MESH = pl.DeviceIdType.MESH
GROUPS = ((0, 4), (4, 3), (7, 1))


def kernel(
    vis_hbm, okay_hbm, tri_hbm, means_ref, closure_ref,
    vis, okay, tri, mask, table, ask, asked, own_pq, own_pr,
    s_asked, s_pq, s_pr,
    edge_a, edge_b, product, give, got, split, part, arrived, spec, spec_in,
    load_sem, vis_sem, smem_sem, ask_send, ask_recv, row_send, row_recv,
    mean_send, mean_recv, spec_send, spec_recv,
):
    tile = lax.axis_index("tile")
    grp = lax.axis_index("grp")
    tiles = lax.axis_size("tile")
    grps = lax.axis_size("grp")
    block = vis.shape[1]
    dishes = vis.shape[2]
    quarter = block // 4

    load_tri = pltpu.make_async_copy(tri_hbm, tri, load_sem.at[0])
    load_tri.start()
    load_okay = pltpu.make_async_copy(okay_hbm, okay, load_sem.at[1])
    load_okay.start()
    loads = []
    for k in range(4):
        rows = pl.ds(k * quarter, quarter)
        load = pltpu.make_async_copy(vis_hbm.at[:, rows], vis.at[:, rows], vis_sem.at[k])
        load.start()
        loads.append(load)

    barrier = pltpu.get_barrier_semaphore()
    for k in range(1, tiles):
        pl.semaphore_signal(barrier, inc=1, device_id={"tile": lax.rem(tile + k, tiles)}, device_id_type=MESH)
    for k in range(1, grps):
        pl.semaphore_signal(barrier, inc=1, device_id={"grp": lax.rem(grp + k, grps)}, device_id_type=MESH)

    partner = [tile + 1 - 2 * lax.rem(tile, 2), tile + 2 - 4 * lax.rem(lax.div(tile, 2), 2)]

    load_tri.wait()
    for lvl in range(LEVELS):
        cols = pl.ds(lvl * TRI_LVL, TRI_LVL)
        first = jnp.bitwise_and(tri[0:1, cols], block - 1)
        second = tri[1:2, cols]
        third = tri[2:3, cols]
        own_pq[:, cols] = first * dishes + second
        own_pr[:, cols] = first * dishes + third
        ask[lvl] = jnp.bitwise_and(second, block - 1) * dishes + third
    to_pq = pltpu.make_async_copy(own_pq, s_pq, smem_sem.at[0])
    to_pq.start()
    to_pr = pltpu.make_async_copy(own_pr, s_pr, smem_sem.at[1])
    to_pr.start()

    pl.semaphore_wait(barrier, tiles - 1 + grps - 1)
    asks = []
    for lvl in (1, 0):
        send = pltpu.make_async_remote_copy(
            src_ref=ask.at[lvl], dst_ref=asked.at[lvl],
            send_sem=ask_send.at[lvl], recv_sem=ask_recv.at[lvl],
            device_id={"tile": partner[lvl]}, device_id_type=MESH,
        )
        send.start()
        asks.append(send)

    load_okay.wait()
    flags_t = jnp.transpose(okay[...].astype(jnp.float32)).astype(jnp.bfloat16)

    rows_of = table.reshape(2 * block * dishes, table.shape[2])

    def build_row(p, _):
        pick = (lax.broadcasted_iota(jnp.int32, (block, 128), 0) == p).astype(jnp.float32).astype(jnp.bfloat16)
        mask[...] = jnp.dot(flags_t, pick, preferred_element_type=jnp.float32)

        def build(i, _):
            for u in range(4):
                r = pl.multiple_of((i * 4 + u) * 16, 16)
                keep = mask[pl.ds(r, 16), :]
                base = p * (2 * dishes) + 2 * r
                rows_of[pl.ds(base, 16, stride=2), :] = vis[0, p, pl.ds(r, 16), :].astype(jnp.float32) * keep
                rows_of[pl.ds(base + 1, 16, stride=2), :] = vis[1, p, pl.ds(r, 16), :].astype(jnp.float32) * keep
            return 0

        lax.fori_loop(0, dishes // 64, build, 0)
        return 0

    for k in range(4):
        loads[k].wait()
        lax.fori_loop(k * quarter, (k + 1) * quarter, build_row, 0)
    to_pq.wait()
    to_pr.wait()

    def gather(index, start, dst):
        def body(g, _):
            for u in range(UNROLL):
                j = g * UNROLL + u
                dst[pl.ds(pl.multiple_of(2 * j, 2), 2), :] = table[index(start + j)]
            return 0

        lax.fori_loop(0, CHUNK // UNROLL, body, 0)

    def own(piece):
        gather(lambda j: s_pq[0, j], piece * CHUNK, edge_a)
        gather(lambda j: s_pr[0, j], piece * CHUNK, edge_b)

        def body(g, _):
            r = pl.multiple_of(g * 32, 32)
            a_re = edge_a[pl.ds(r, 16, stride=2), :]
            a_im = edge_a[pl.ds(r + 1, 16, stride=2), :]
            b_re = edge_b[pl.ds(r, 16, stride=2), :]
            b_im = edge_b[pl.ds(r + 1, 16, stride=2), :]
            at = pl.ds(pl.multiple_of(g * 16, 16), 16)
            product[piece, 0, at, :] = a_re * b_re + a_im * b_im
            product[piece, 1, at, :] = a_im * b_re - a_re * b_im
            return 0

        lax.fori_loop(0, CHUNK // 16, body, 0)

    def serve(lvl, chunk):
        piece = lvl * CHUNKS + chunk
        gather(lambda j: s_asked[lvl, 0, j], chunk * CHUNK, edge_a)

        def body(g, _):
            r = pl.multiple_of(g * 32, 32)
            at = pl.ds(pl.multiple_of(g * 16, 16), 16)
            give[piece, 0, at, :] = edge_a[pl.ds(r, 16, stride=2), :].astype(jnp.bfloat16)
            give[piece, 1, at, :] = edge_a[pl.ds(r + 1, 16, stride=2), :].astype(jnp.bfloat16)
            return 0

        lax.fori_loop(0, CHUNK // 16, body, 0)
        send = pltpu.make_async_remote_copy(
            src_ref=give.at[piece], dst_ref=got.at[piece],
            send_sem=row_send.at[piece], recv_sem=row_recv.at[piece],
            device_id={"tile": partner[lvl]}, device_id_type=MESH,
        )
        send.start()
        return send

    ones = jnp.ones((8, 128), jnp.bfloat16)

    def combine(piece, sums):
        def body(g, sums):
            at = pl.ds(pl.multiple_of(g * 16, 16), 16)
            p_re = product[piece, 0, at, :]
            p_im = product[piece, 1, at, :]
            c_re = got[piece, 0, at, :].astype(jnp.float32)
            c_im = got[piece, 1, at, :].astype(jnp.float32)
            re = p_re * c_re - p_im * c_im
            im = p_re * c_im + p_im * c_re
            mag = jnp.sqrt(re * re + im * im)
            re_hi = re.astype(jnp.bfloat16)
            im_hi = im.astype(jnp.bfloat16)
            split[0, at, :] = re_hi
            split[1, at, :] = (re - re_hi.astype(jnp.float32)).astype(jnp.bfloat16)
            split[2, at, :] = im_hi
            split[3, at, :] = (im - im_hi.astype(jnp.float32)).astype(jnp.bfloat16)
            return (
                sums[0] + re[:8] + re[8:],
                sums[1] + im[:8] + im[8:],
                sums[2] + mag[:8] + mag[8:],
            )

        sums = lax.fori_loop(0, CHUNK // 16, body, sums)

        def lanes(k):
            return lax.dot_general(ones, split[k], (((1,), (1,)), ((), ())), preferred_element_type=jnp.float32)

        part[piece, 0:1, :] = (lanes(0) + lanes(1))[0:1]
        part[piece, 1:2, :] = (lanes(2) + lanes(3))[0:1]
        arrived[0, piece] = part[piece]
        return sums

    def share(n):
        start, count = GROUPS[n]
        sends = []
        for k in range(1, grps):
            send = pltpu.make_async_remote_copy(
                src_ref=part.at[pl.ds(start, count)], dst_ref=arrived.at[k, pl.ds(start, count)],
                send_sem=mean_send.at[n, k - 1], recv_sem=mean_recv.at[n, k - 1],
                device_id={"grp": lax.rem(grp + k, grps)}, device_id_type=MESH,
            )
            send.start()
            sends.append(send)
        return sends

    def index_in(lvl):
        asks[1 - lvl].wait_recv()
        copy = pltpu.make_async_copy(asked.at[lvl], s_asked.at[lvl], smem_sem.at[2 + lvl])
        copy.start()
        return copy

    index_in(1).wait()
    sends = [serve(1, c) for c in range(CHUNKS)]
    index_in(0).wait()
    sends0 = [serve(0, c) for c in range(CHUNKS)]
    zero = jnp.zeros((8, 128), jnp.float32)
    sums = (zero, zero, zero)
    for c in range(CHUNKS):
        own(c)
    for c in range(CHUNKS):
        sends0[c].wait_recv()
        sums = combine(c, sums)
    mean_sends = share(0)
    for c in range(CHUNKS):
        own(CHUNKS + c)
    for c in range(CHUNKS):
        sends[c].wait_recv()
        sums = combine(CHUNKS + c, sums)
        if c == CHUNKS - 2:
            mean_sends += share(1)
    mean_sends += share(2)

    for k in range(3):
        spec[k : k + 1, :] = jnp.sum(sums[k], axis=0, keepdims=True)
    spec[3:4, :] = jnp.zeros((1, 128), jnp.float32)
    spec_in[0] = spec[...]
    spec_sends = []
    for k in range(1, tiles):
        send = pltpu.make_async_remote_copy(
            src_ref=spec, dst_ref=spec_in.at[k],
            send_sem=spec_send.at[k - 1], recv_sem=spec_recv.at[k - 1],
            device_id={"tile": lax.rem(tile + k, tiles)}, device_id_type=MESH,
        )
        send.start()
        spec_sends.append(send)

    def finish(n):
        start, count = GROUPS[n]
        for send in mean_sends[n * (grps - 1) : (n + 1) * (grps - 1)]:
            send.wait_recv()
        total = arrived[lax.rem(grp + grps, grps), pl.ds(start, count)]
        for s in range(1, grps):
            total = total + arrived[lax.rem(grp - s + grps, grps), pl.ds(start, count)]
        total = total * (1.0 / RADIO_BANDS)
        for c in range(count):
            means_ref[:, pl.ds((start + c) * CHUNK, CHUNK)] = total[c]

    for n in range(len(GROUPS)):
        finish(n)
    for send in spec_sends:
        send.wait_recv()
    total = jnp.sum(spec_in[...], axis=0)
    closure_ref[...] = total[0:2] / (1.0 + total[2:3])

    for send in asks + sends + sends0 + mean_sends + spec_sends:
        send.wait_send()


def fused(visibility, dish_pair_okay, triangles):
    block, dishes, channels = visibility.shape[1:]
    tiles = lax.axis_size("tile")
    grps = lax.axis_size("grp")
    f32, bf16, i32 = jnp.float32, jnp.bfloat16, jnp.int32
    groups = len(GROUPS)
    dma = pltpu.SemaphoreType.DMA
    return pl.pallas_call(
        kernel,
        out_shape=(
            jax.ShapeDtypeStruct((2, LEVELS * TRI_LVL), f32),
            jax.ShapeDtypeStruct((2, channels), f32),
        ),
        in_specs=[pl.BlockSpec(memory_space=pl.ANY)] * 3,
        out_specs=(pl.BlockSpec(memory_space=pltpu.VMEM), pl.BlockSpec(memory_space=pltpu.VMEM)),
        scratch_shapes=[
            pltpu.VMEM((2, block, dishes, channels), bf16),
            pltpu.VMEM((block, dishes), i32),
            pltpu.VMEM((3, LEVELS * TRI_LVL), i32),
            pltpu.VMEM((dishes, channels), f32),
            pltpu.VMEM((block * dishes, 2, channels), f32),
            pltpu.VMEM((LEVELS, 1, TRI_LVL), i32),
            pltpu.VMEM((LEVELS, 1, TRI_LVL), i32),
            pltpu.VMEM((1, LEVELS * TRI_LVL), i32),
            pltpu.VMEM((1, LEVELS * TRI_LVL), i32),
            pltpu.SMEM((LEVELS, 1, TRI_LVL), i32),
            pltpu.SMEM((1, LEVELS * TRI_LVL), i32),
            pltpu.SMEM((1, LEVELS * TRI_LVL), i32),
            pltpu.VMEM((2 * CHUNK, channels), f32),
            pltpu.VMEM((2 * CHUNK, channels), f32),
            pltpu.VMEM((PIECES, 2, CHUNK, channels), f32),
            pltpu.VMEM((PIECES, 2, CHUNK, channels), bf16),
            pltpu.VMEM((PIECES, 2, CHUNK, channels), bf16),
            pltpu.VMEM((4, CHUNK, channels), bf16),
            pltpu.VMEM((PIECES, 2, CHUNK), f32),
            pltpu.VMEM((grps, PIECES, 2, CHUNK), f32),
            pltpu.VMEM((4, channels), f32),
            pltpu.VMEM((tiles, 4, channels), f32),
            dma((2,)), dma((4,)), dma((4,)),
            dma((LEVELS,)), dma((LEVELS,)),
            dma((PIECES,)), dma((PIECES,)),
            dma((groups, grps - 1)), dma((groups, grps - 1)),
            dma((tiles - 1,)), dma((tiles - 1,)),
        ],
        compiler_params=pltpu.CompilerParams(collective_id=0, has_side_effects=True, vmem_limit_bytes=48 * 2**20),
        name="closure",
    )(visibility, dish_pair_okay, triangles)


def body(visibility, dish_pair_okay, triangles):
    means, closure = fused(visibility, dish_pair_okay, triangles)
    tile = lax.axis_index("tile")
    width = closure.shape[1] // lax.axis_size("tile")
    return means, lax.dynamic_slice(closure, (0, tile * width), (2, width))


def solution(mesh):
    placed = (P(None, "tile", None, "grp"), P("tile", None), P(None, "tile"))
    return jax.shard_map(
        body,
        mesh=mesh,
        in_specs=placed,
        out_specs=(P(None, "tile"), P(None, ("grp", "tile"))),
        check_vma=False,
    )
```

```python
import jax
import jax.numpy as jnp
from jax import lax
from jax.experimental import pallas as pl
from jax.experimental.pallas import tpu as pltpu
from jax.sharding import PartitionSpec as P

RADIO_BANDS = 1024
TRI_LVL = 1024
LEVELS = 2
CHUNK = 128
CHUNKS = TRI_LVL // CHUNK
PIECES = LEVELS * CHUNKS
UNROLL = 32
MESH = pl.DeviceIdType.MESH
NEAR = ((1, 0, 0, 0), (-1, 0, 0, 0), (0, 1, 0, 0), (0, -1, 0, 0), (0, 0, 1, 0), (0, 0, -1, 0), (0, 0, 0, 1))
SECOND = ((0, 0, 0, 1), (2, 0, 0, 0), (0, 2, 0, 0), (0, 0, 2, 0), (0, 0, -2, 0))
THIRD = ((0, 0, 2, 0), (0, 0, -2, 0))
GROUPS = ((0, 8), (8, 7), (15, 1))


def kernel(
    vis_hbm, okay_hbm, tri_hbm, means_ref, closure_ref,
    vis, okay, tri, mask, table, ask, asked, own_pq, own_pr,
    s_asked0, s_asked1, s_pq, s_pr,
    edge_a, edge_b, product, give, got, split, part, arrived, spec, spec_in,
    known, load_sem, vis_sem, smem_sem, ask_send, ask_recv, row_send, row_recv,
    mean_send, mean_recv, spec_send, spec_recv,
):
    tile = lax.axis_index("tile")
    grp = lax.axis_index("grp")
    tiles = lax.axis_size("tile")
    grps = lax.axis_size("grp")
    block = vis.shape[1]
    dishes = vis.shape[2]
    quarter = block // 4

    load_tri = pltpu.make_async_copy(tri_hbm, tri, load_sem.at[0])
    load_tri.start()
    load_okay = pltpu.make_async_copy(okay_hbm, okay, load_sem.at[1])
    load_okay.start()
    loads = []
    for k in range(4):
        rows = pl.ds(k * quarter, quarter)
        load = pltpu.make_async_copy(vis_hbm.at[:, rows], vis.at[:, rows], vis_sem.at[k])
        load.start()
        loads.append(load)

    barrier = pltpu.get_barrier_semaphore()
    spots = (lax.rem(grp, 4), lax.rem(lax.div(tile, 2), 4), lax.div(grp, 4) * 4 + lax.div(tile, 8), lax.rem(tile, 2))

    def tell(sem, steps):
        for step in steps:
            x, y, z, core = (lax.rem(at + d + n, n) for at, d, n in zip(spots, step, (4, 4, 8, 2)))
            there = {"grp": lax.div(z, 4) * 4 + x, "tile": lax.rem(z, 4) * 8 + y * 2 + core}
            pl.semaphore_signal(sem, inc=1, device_id=there, device_id_type=MESH)

    tell(barrier, NEAR)
    s_asked = (s_asked0, s_asked1)

    partner = [tile + 1 - 2 * lax.rem(tile, 2), tile + 2 - 4 * lax.rem(lax.div(tile, 2), 2)]

    load_tri.wait()
    for lvl in range(LEVELS):
        cols = pl.ds(lvl * TRI_LVL, TRI_LVL)
        first = jnp.bitwise_and(tri[0:1, cols], block - 1)
        second = tri[1:2, cols]
        third = tri[2:3, cols]
        own_pq[:, cols] = first * dishes + second
        own_pr[:, cols] = first * dishes + third
        ask[lvl] = jnp.bitwise_and(second, block - 1) * dishes + third
    to_pq = pltpu.make_async_copy(own_pq, s_pq, smem_sem.at[0])
    to_pq.start()
    to_pr = pltpu.make_async_copy(own_pr, s_pr, smem_sem.at[1])
    to_pr.start()

    pl.semaphore_wait(barrier, len(NEAR))
    tell(known.at[0], NEAR)
    asks = []
    for lvl in (1, 0):
        send = pltpu.make_async_remote_copy(
            src_ref=ask.at[lvl], dst_ref=asked.at[lvl],
            send_sem=ask_send.at[lvl], recv_sem=ask_recv.at[lvl],
            device_id={"tile": partner[lvl]}, device_id_type=MESH,
        )
        send.start()
        asks.append(send)

    load_okay.wait()
    flags_t = jnp.transpose(okay[...].astype(jnp.float32)).astype(jnp.bfloat16)

    rows_of = table.reshape(2 * block * dishes, table.shape[2])

    def build_row(p, _):
        pick = (lax.broadcasted_iota(jnp.int32, (block, 128), 0) == p).astype(jnp.float32).astype(jnp.bfloat16)
        mask[...] = jnp.dot(flags_t, pick, preferred_element_type=jnp.float32)

        def build(i, _):
            for u in range(4):
                r = pl.multiple_of((i * 4 + u) * 16, 16)
                keep = mask[pl.ds(r, 16), :]
                base = p * (2 * dishes) + 2 * r
                rows_of[pl.ds(base, 16, stride=2), :] = vis[0, p, pl.ds(r, 16), :].astype(jnp.float32) * keep
                rows_of[pl.ds(base + 1, 16, stride=2), :] = vis[1, p, pl.ds(r, 16), :].astype(jnp.float32) * keep
            return 0

        lax.fori_loop(0, dishes // 64, build, 0)
        return 0

    for k in range(4):
        loads[k].wait()
        lax.fori_loop(k * quarter, (k + 1) * quarter, build_row, 0)
    to_pq.wait()
    to_pr.wait()

    def gather(index, start, dst):
        def body(g, _):
            for u in range(UNROLL):
                j = g * UNROLL + u
                dst[pl.ds(pl.multiple_of(2 * j, 2), 2), :] = table[index(start + j)]
            return 0

        lax.fori_loop(0, CHUNK // UNROLL, body, 0)

    def own(piece):
        gather(lambda j: s_pq[0, j], piece * CHUNK, edge_a)
        gather(lambda j: s_pr[0, j], piece * CHUNK, edge_b)

        def body(g, _):
            r = pl.multiple_of(g * 32, 32)
            a_re = edge_a[pl.ds(r, 16, stride=2), :]
            a_im = edge_a[pl.ds(r + 1, 16, stride=2), :]
            b_re = edge_b[pl.ds(r, 16, stride=2), :]
            b_im = edge_b[pl.ds(r + 1, 16, stride=2), :]
            at = pl.ds(pl.multiple_of(g * 16, 16), 16)
            product[piece, 0, at, :] = a_re * b_re + a_im * b_im
            product[piece, 1, at, :] = a_im * b_re - a_re * b_im
            return 0

        lax.fori_loop(0, CHUNK // 16, body, 0)

    def serve(lvl, chunk):
        piece = lvl * CHUNKS + chunk
        gather(lambda j: s_asked[lvl][0, j], chunk * CHUNK, edge_a)

        def body(g, _):
            r = pl.multiple_of(g * 32, 32)
            at = pl.ds(pl.multiple_of(g * 16, 16), 16)
            give[piece, 0, at, :] = edge_a[pl.ds(r, 16, stride=2), :].astype(jnp.bfloat16)
            give[piece, 1, at, :] = edge_a[pl.ds(r + 1, 16, stride=2), :].astype(jnp.bfloat16)
            return 0

        lax.fori_loop(0, CHUNK // 16, body, 0)
        send = pltpu.make_async_remote_copy(
            src_ref=give.at[piece], dst_ref=got.at[piece],
            send_sem=row_send.at[piece], recv_sem=row_recv.at[piece],
            device_id={"tile": partner[lvl]}, device_id_type=MESH,
        )
        send.start()
        return send

    ones = jnp.ones((8, 128), jnp.bfloat16)

    def combine(piece, sums):
        def body(g, sums):
            at = pl.ds(pl.multiple_of(g * 16, 16), 16)
            p_re = product[piece, 0, at, :]
            p_im = product[piece, 1, at, :]
            c_re = got[piece, 0, at, :].astype(jnp.float32)
            c_im = got[piece, 1, at, :].astype(jnp.float32)
            re = p_re * c_re - p_im * c_im
            im = p_re * c_im + p_im * c_re
            mag = jnp.sqrt(re * re + im * im)
            re_hi = re.astype(jnp.bfloat16)
            im_hi = im.astype(jnp.bfloat16)
            split[0, at, :] = re_hi
            split[1, at, :] = (re - re_hi.astype(jnp.float32)).astype(jnp.bfloat16)
            split[2, at, :] = im_hi
            split[3, at, :] = (im - im_hi.astype(jnp.float32)).astype(jnp.bfloat16)
            return (
                sums[0] + re[:8] + re[8:],
                sums[1] + im[:8] + im[8:],
                sums[2] + mag[:8] + mag[8:],
            )

        sums = lax.fori_loop(0, CHUNK // 16, body, sums)

        def lanes(k):
            return lax.dot_general(ones, split[k], (((1,), (1,)), ((), ())), preferred_element_type=jnp.float32)

        part[piece, 0:1, :] = (lanes(0) + lanes(1))[0:1]
        part[piece, 1:2, :] = (lanes(2) + lanes(3))[0:1]
        arrived[0, piece] = part[piece]
        return sums

    def share(n):
        start, count = GROUPS[n]
        sends = []
        for k in range(1, grps):
            send = pltpu.make_async_remote_copy(
                src_ref=part.at[pl.ds(start, count)], dst_ref=arrived.at[k, pl.ds(start, count)],
                send_sem=mean_send.at[n, k - 1], recv_sem=mean_recv.at[n, k - 1],
                device_id={"grp": lax.rem(grp + k, grps)}, device_id_type=MESH,
            )
            send.start()
            sends.append(send)
        return sends

    def index_in(lvl):
        asks[1 - lvl].wait_recv()
        copy = pltpu.make_async_copy(asked.at[lvl], s_asked[lvl], smem_sem.at[2 + lvl])
        copy.start()
        return copy

    index_in(1).wait()
    sends = [serve(1, c) for c in range(CHUNKS)]
    pl.semaphore_wait(known.at[0], len(NEAR))
    tell(known.at[1], SECOND)
    index_in(0).wait()
    sends0 = [serve(0, c) for c in range(CHUNKS)]
    pl.semaphore_wait(known.at[1], len(SECOND))
    tell(known.at[2], THIRD)
    zero = jnp.zeros((8, 128), jnp.float32)
    sums = (zero, zero, zero)
    for c in range(CHUNKS):
        own(c)
    for c in range(CHUNKS):
        sends0[c].wait_recv()
        sums = combine(c, sums)
    pl.semaphore_wait(known.at[2], len(THIRD))
    mean_sends = share(0)
    for c in range(CHUNKS):
        own(CHUNKS + c)
    for c in range(CHUNKS):
        sends[c].wait_recv()
        sums = combine(CHUNKS + c, sums)
        if c == CHUNKS - 2:
            mean_sends += share(1)
    mean_sends += share(2)

    for k in range(3):
        spec[k : k + 1, :] = jnp.sum(sums[k], axis=0, keepdims=True)
    spec[3:4, :] = jnp.zeros((1, 128), jnp.float32)
    spec_in[0] = spec[...]
    spec_sends = []
    for k in range(1, tiles):
        send = pltpu.make_async_remote_copy(
            src_ref=spec, dst_ref=spec_in.at[k],
            send_sem=spec_send.at[k - 1], recv_sem=spec_recv.at[k - 1],
            device_id={"tile": lax.rem(tile + k, tiles)}, device_id_type=MESH,
        )
        send.start()
        spec_sends.append(send)

    def finish(n):
        start, count = GROUPS[n]
        for send in mean_sends[n * (grps - 1) : (n + 1) * (grps - 1)]:
            send.wait_recv()
        total = arrived[lax.rem(grp + grps, grps), pl.ds(start, count)]
        for s in range(1, grps):
            total = total + arrived[lax.rem(grp - s + grps, grps), pl.ds(start, count)]
        total = total * (1.0 / RADIO_BANDS)
        for c in range(count):
            means_ref[:, pl.ds((start + c) * CHUNK, CHUNK)] = total[c]

    for n in range(len(GROUPS)):
        finish(n)
    for send in spec_sends:
        send.wait_recv()
    total = jnp.sum(spec_in[...], axis=0)
    closure_ref[...] = total[0:2] / (1.0 + total[2:3])

    for send in asks + sends + sends0 + mean_sends + spec_sends:
        send.wait_send()


def fused(visibility, dish_pair_okay, triangles):
    block, dishes, channels = visibility.shape[1:]
    tiles = lax.axis_size("tile")
    grps = lax.axis_size("grp")
    f32, bf16, i32 = jnp.float32, jnp.bfloat16, jnp.int32
    groups = len(GROUPS)
    dma = pltpu.SemaphoreType.DMA
    return pl.pallas_call(
        kernel,
        out_shape=(
            jax.ShapeDtypeStruct((2, LEVELS * TRI_LVL), f32),
            jax.ShapeDtypeStruct((2, channels), f32),
        ),
        in_specs=[pl.BlockSpec(memory_space=pltpu.HBM)] * 3,
        out_specs=(pl.BlockSpec(memory_space=pltpu.VMEM), pl.BlockSpec(memory_space=pltpu.VMEM)),
        scratch_shapes=[
            pltpu.VMEM((2, block, dishes, channels), bf16),
            pltpu.VMEM((block, dishes), i32),
            pltpu.VMEM((3, LEVELS * TRI_LVL), i32),
            pltpu.VMEM((dishes, channels), f32),
            pltpu.VMEM((block * dishes, 2, channels), f32),
            pltpu.VMEM((LEVELS, 1, TRI_LVL), i32),
            pltpu.VMEM((LEVELS, 1, TRI_LVL), i32),
            pltpu.VMEM((1, LEVELS * TRI_LVL), i32),
            pltpu.VMEM((1, LEVELS * TRI_LVL), i32),
            pltpu.SMEM((1, TRI_LVL), i32),
            pltpu.SMEM((1, TRI_LVL), i32),
            pltpu.SMEM((1, LEVELS * TRI_LVL), i32),
            pltpu.SMEM((1, LEVELS * TRI_LVL), i32),
            pltpu.VMEM((2 * CHUNK, channels), f32),
            pltpu.VMEM((2 * CHUNK, channels), f32),
            pltpu.VMEM((PIECES, 2, CHUNK, channels), f32),
            pltpu.VMEM((PIECES, 2, CHUNK, channels), bf16),
            pltpu.VMEM((PIECES, 2, CHUNK, channels), bf16),
            pltpu.VMEM((4, CHUNK, channels), bf16),
            pltpu.VMEM((PIECES, 2, CHUNK), f32),
            pltpu.VMEM((grps, PIECES, 2, CHUNK), f32),
            pltpu.VMEM((4, channels), f32),
            pltpu.VMEM((tiles, 4, channels), f32),
            pltpu.SemaphoreType.REGULAR((3,)),
            dma((2,)), dma((4,)), dma((4,)),
            dma((LEVELS,)), dma((LEVELS,)),
            dma((PIECES,)), dma((PIECES,)),
            dma((groups, grps - 1)), dma((groups, grps - 1)),
            dma((tiles - 1,)), dma((tiles - 1,)),
        ],
        compiler_params=pltpu.CompilerParams(collective_id=0, has_side_effects=True, vmem_limit_bytes=67043328),
        name="closure",
    )(visibility, dish_pair_okay, triangles)


def body(visibility, dish_pair_okay, triangles):
    means, closure = fused(visibility, dish_pair_okay, triangles)
    tile = lax.axis_index("tile")
    width = closure.shape[1] // lax.axis_size("tile")
    return means, lax.dynamic_slice(closure, (0, tile * width), (2, width))


def solution(mesh):
    placed = (P(None, "tile", None, "grp"), P("tile", None), P(None, "tile"))
    return jax.shard_map(
        body,
        mesh=mesh,
        in_specs=placed,
        out_specs=(P(None, "tile"), P(None, ("grp", "tile"))),
        check_vma=False,
    )
```

```python
import jax
import jax.numpy as jnp
from jax import lax
from jax.experimental import pallas as pl
from jax.experimental.pallas import tpu as pltpu
from jax.sharding import PartitionSpec as P

RADIO_BANDS = 1024
TRI_LVL = 1024
LEVELS = 2
CHUNK = 128
CHUNKS = TRI_LVL // CHUNK
PIECES = LEVELS * CHUNKS
UNROLL = 32
EARLY_ROWS = 12
MESH = pl.DeviceIdType.MESH
NEAR = ((1, 0, 0, 0), (-1, 0, 0, 0), (0, 1, 0, 0), (0, -1, 0, 0), (0, 0, 1, 0), (0, 0, -1, 0), (0, 0, 0, 1))
SECOND = ((0, 0, 0, 1), (2, 0, 0, 0), (0, 2, 0, 0), (0, 0, 2, 0), (0, 0, -2, 0))
THIRD = ((0, 0, 2, 0), (0, 0, -2, 0))
GROUPS = ((0, 8), (8, 4), (12, 2), (14, 1), (15, 1))


def kernel(
    vis_hbm, okay_hbm, tri_hbm, means_ref, closure_ref,
    vis, okay, tri, mask, table, ask, asked, own_pr, s_asked0, s_asked1, s_pr,
    edge_ab, edge_bc, edge_ac, product, give, got, split, spec, spec_in, part, arrived,
    known, load_sem, vis_sem, smem_sem, ask_send, ask_recv, row_send, row_recv,
    mean_send, mean_recv, spec_send, spec_recv,
):
    f32, bf16 = jnp.float32, jnp.bfloat16
    tile = lax.axis_index("tile")
    grp = lax.axis_index("grp")
    tiles = lax.axis_size("tile")
    grps = lax.axis_size("grp")
    block, dishes, channels = vis.shape[1:]
    s_asked = (s_asked0, s_asked1)

    load_tri = pltpu.make_async_copy(tri_hbm, tri, load_sem.at[0])
    load_tri.start()
    load_okay = pltpu.make_async_copy(okay_hbm, okay, load_sem.at[1])
    load_okay.start()

    def load_row(p):
        return pltpu.make_async_copy(vis_hbm.at[:, p], vis.at[:, p], vis_sem.at[p])

    for p in range(block):
        load_row(p).start()

    barrier = pltpu.get_barrier_semaphore()
    spots = (lax.rem(grp, 4), lax.rem(lax.div(tile, 2), 4), lax.div(grp, 4) * 4 + lax.div(tile, 8), lax.rem(tile, 2))

    def tell(sem, steps):
        for step in steps:
            x, y, z, core = (lax.rem(at + d + n, n) for at, d, n in zip(spots, step, (4, 4, 8, 2)))
            there = {"grp": lax.div(z, 4) * 4 + x, "tile": lax.rem(z, 4) * 8 + y * 2 + core}
            pl.semaphore_signal(sem, inc=1, device_id=there, device_id_type=MESH)

    tell(barrier, NEAR)
    partner = [tile + 1 - 2 * lax.rem(tile, 2), tile + 2 - 4 * lax.rem(lax.div(tile, 2), 2)]

    with jax.named_scope("tri_wait"):
        load_tri.wait()
    first = jnp.bitwise_and(tri[0:1, :], block - 1)
    second = jnp.bitwise_and(tri[1:2, :], block - 1)
    third = tri[2:3, :]
    wanted = second * dishes + third
    for lvl in range(LEVELS):
        ask[lvl] = wanted[:, lvl * TRI_LVL : (lvl + 1) * TRI_LVL]

    with jax.named_scope("barrier"):
        pl.semaphore_wait(barrier, len(NEAR))
    tell(known.at[0], NEAR)
    asks = []
    for lvl in range(LEVELS):
        asks.append(
            pltpu.make_async_remote_copy(
                src_ref=ask.at[lvl], dst_ref=asked.at[lvl],
                send_sem=ask_send.at[lvl], recv_sem=ask_recv.at[lvl],
                device_id={"tile": partner[lvl]}, device_id_type=MESH,
            )
        )
    asks[1].start()
    asks[0].start()
    own_pr[...] = first * dishes + third
    to_pr = pltpu.make_async_copy(own_pr, s_pr, smem_sem.at[2])
    to_pr.start()
    pair = (first * block + second).astype(f32)

    with jax.named_scope("flags"):
        load_okay.wait()
        flags_t = jnp.transpose(okay[...].astype(f32)).astype(bf16)
        for c in range(0, block, 2):
            row = lax.broadcasted_iota(jnp.int32, (block, 2 * channels), 0)
            col = lax.broadcasted_iota(jnp.int32, (block, 2 * channels), 1)
            pick = jnp.where(row == c + (col >= channels).astype(jnp.int32), 1.0, 0.0).astype(bf16)
            both = jnp.dot(flags_t, pick, preferred_element_type=f32).astype(bf16)
            mask[c] = both[:, :channels]
            mask[c + 1] = both[:, channels:]

    flat = table.reshape(2 * block * dishes, channels)

    def build(p, _):
        load_row(p).wait()
        for r in range(0, dishes, 16):
            keep = mask[p, r : r + 16, :]
            base = p * (2 * dishes) + 2 * r
            flat[pl.ds(base, 16, stride=2), :] = (vis[0, p, r : r + 16, :] * keep).astype(f32)
            flat[pl.ds(base + 1, 16, stride=2), :] = (vis[1, p, r : r + 16, :] * keep).astype(f32)
        return 0

    with jax.named_scope("build"):
        lax.fori_loop(0, EARLY_ROWS, build, 0)
    to_asked = []
    with jax.named_scope("ask_wait"):
        for lvl in (1, 0):
            asks[lvl].wait_recv()
            copy = pltpu.make_async_copy(asked.at[lvl], s_asked[lvl], smem_sem.at[lvl])
            copy.start()
            to_asked.append(copy)
    with jax.named_scope("build_late"):
        lax.fori_loop(EARLY_ROWS, block, build, 0)

    def gather(index, start, dst):
        def body(g, _):
            for u in range(UNROLL):
                j = g * UNROLL + u
                dst[pl.ds(pl.multiple_of(2 * j, 2), 2), :] = table[index[0, start + j]]
            return 0

        lax.fori_loop(0, CHUNK // UNROLL, body, 0)

    def serve(lvl, chunk):
        piece = lvl * CHUNKS + chunk
        gather(s_asked[lvl], chunk * CHUNK, edge_bc)
        for r in range(0, CHUNK, 16):
            give[piece, 0, r : r + 16, :] = edge_bc[pl.ds(2 * r, 16, stride=2), :].astype(bf16)
            give[piece, 1, r : r + 16, :] = edge_bc[pl.ds(2 * r + 1, 16, stride=2), :].astype(bf16)
        send = pltpu.make_async_remote_copy(
            src_ref=give.at[piece], dst_ref=got.at[piece],
            send_sem=row_send.at[piece], recv_sem=row_recv.at[piece],
            device_id={"tile": partner[lvl]}, device_id_type=MESH,
        )
        send.start()
        return send

    def own(lvl):
        start = pl.multiple_of(partner[lvl] * block, block)
        for p in range(block):
            keep = mask[p, pl.ds(start, block), :]
            at = slice(p * block, (p + 1) * block)
            edge_ab[at, :channels] = vis[0, p, pl.ds(start, block), :] * keep
            edge_ab[at, channels:] = vis[1, p, pl.ds(start, block), :] * keep
        codes = [pair[:, (lvl * CHUNKS + c) * CHUNK : (lvl * CHUNKS + c + 1) * CHUNK] for c in range(CHUNKS)]
        codes_t = jnp.transpose(jnp.concatenate(codes, axis=0))
        lane = lax.broadcasted_iota(jnp.int32, (CHUNK, block * block), 1).astype(f32)
        for c in range(CHUNKS):
            piece = lvl * CHUNKS + c
            hot = jnp.where(lane == codes_t[:, c : c + 1], 1.0, 0.0).astype(bf16)
            ab = jnp.dot(hot, edge_ab[...], preferred_element_type=f32)
            gather(s_pr, piece * CHUNK, edge_ac)
            for r in range(0, CHUNK, 16):
                a_re = ab[r : r + 16, :channels]
                a_im = ab[r : r + 16, channels:]
                b_re = edge_ac[pl.ds(2 * r, 16, stride=2), :]
                b_im = edge_ac[pl.ds(2 * r + 1, 16, stride=2), :]
                product[piece, 0, r : r + 16, :] = a_re * b_re + a_im * b_im
                product[piece, 1, r : r + 16, :] = a_im * b_re - a_re * b_im

    def combine(piece, row, sums, total):
        slot = piece % 2

        def body(g, sums):
            at = pl.ds(pl.multiple_of(g * 16, 16), 16)
            low = pl.ds(pl.multiple_of(CHUNK + g * 16, 16), 16)
            p_re = product[piece, 0, at, :]
            p_im = product[piece, 1, at, :]
            c_re = got[piece, 0, at, :].astype(f32)
            c_im = got[piece, 1, at, :].astype(f32)
            re = p_re * c_re - p_im * c_im
            im = p_re * c_im + p_im * c_re
            mag = jnp.sqrt(re * re + im * im)
            re_hi = re.astype(bf16)
            im_hi = im.astype(bf16)
            split[slot, at, :channels] = re_hi
            split[slot, at, channels:] = (re - re_hi.astype(f32)).astype(bf16)
            split[slot, low, :channels] = im_hi
            split[slot, low, channels:] = (im - im_hi.astype(f32)).astype(bf16)
            return (
                sums[0] + (re[:8] + re[8:]),
                sums[1] + (im[:8] + im[8:]),
                sums[2] + (mag[:8] + mag[8:]),
            )

        sums = lax.fori_loop(0, CHUNK // 16, body, sums)
        ones = jnp.where(lax.broadcasted_iota(jnp.int32, (8, 2 * channels), 0) == row, 1.0, 0.0).astype(bf16)
        lanes = lax.dot_general(ones, split[slot], (((1,), (1,)), ((), ())), preferred_element_type=f32)
        return sums, lanes if total is None else total + lanes

    def share(n, total):
        count = GROUPS[n][1]
        part[n][...] = total[:count]
        arrived[n][0] = total[:count]
        sends = []
        for k in range(1, grps):
            send = pltpu.make_async_remote_copy(
                src_ref=part[n], dst_ref=arrived[n].at[k],
                send_sem=mean_send.at[n, k - 1], recv_sem=mean_recv.at[n, k - 1],
                device_id={"grp": lax.rem(grp + k, grps)}, device_id_type=MESH,
            )
            send.start()
            sends.append(send)
        return sends

    for copy in to_asked[:1]:
        copy.wait()
    rows = [None] * LEVELS
    with jax.named_scope("serve1"):
        rows[1] = [serve(1, c) for c in range(CHUNKS)]
    with jax.named_scope("known0"):
        pl.semaphore_wait(known.at[0], len(NEAR))
    tell(known.at[1], SECOND)
    to_asked[1].wait()
    with jax.named_scope("serve0"):
        rows[0] = [serve(0, c) for c in range(CHUNKS)]
    to_pr.wait()
    zero = jnp.zeros((8, channels), f32)
    sums = (zero, zero, zero)
    mean_sends = []
    for lvl in range(LEVELS):
        with jax.named_scope(f"own{lvl}"):
            own(lvl)
        if lvl == 0:
            with jax.named_scope("known1"):
                pl.semaphore_wait(known.at[1], len(SECOND))
            tell(known.at[2], THIRD)
        for n, (start, count) in enumerate(GROUPS):
            if start // CHUNKS != lvl:
                continue
            total = None
            for k in range(count):
                piece = start + k
                with jax.named_scope(f"rows{lvl}"):
                    rows[lvl][piece % CHUNKS].wait_recv()
                with jax.named_scope(f"combine{lvl}"):
                    sums, total = combine(piece, k, sums, total)
            if n == 0:
                with jax.named_scope("known2"):
                    pl.semaphore_wait(known.at[2], len(THIRD))
            with jax.named_scope("share"):
                mean_sends.append(share(n, total))

    with jax.named_scope("spec_send"):
        for k in range(3):
            spec[k : k + 1, :] = jnp.sum(sums[k], axis=0, keepdims=True)
        spec[3:4, :] = jnp.zeros((1, channels), f32)
        spec_in[0] = spec[...]
        spec_sends = []
        for k in range(1, tiles):
            send = pltpu.make_async_remote_copy(
                src_ref=spec, dst_ref=spec_in.at[k],
                send_sem=spec_send.at[k - 1], recv_sem=spec_recv.at[k - 1],
                device_id={"tile": lax.rem(tile + k, tiles)}, device_id_type=MESH,
            )
            send.start()
            spec_sends.append(send)

    for n, (start, count) in enumerate(GROUPS):
        with jax.named_scope(f"finish{n}"):
            for send in mean_sends[n]:
                send.wait_recv()
            total = arrived[n][grp]
            for s in range(1, grps):
                total = total + arrived[n][lax.rem(grp - s + grps, grps)]
            total = total * (1.0 / RADIO_BANDS)
            for k in range(count):
                at = slice((start + k) * CHUNK, (start + k + 1) * CHUNK)
                means_ref[0:1, at] = total[k : k + 1, :CHUNK]
                means_ref[1:2, at] = total[k : k + 1, CHUNK:]

    with jax.named_scope("spec_wait"):
        for send in spec_sends:
            send.wait_recv()
        total = jnp.sum(spec_in[...], axis=0)
        closure_ref[...] = total[0:2] / (1.0 + total[2:3])

    with jax.named_scope("send_wait"):
        for send in asks + rows[0] + rows[1] + sum(mean_sends, []) + spec_sends:
            send.wait_send()


def fused(visibility, dish_pair_okay, triangles):
    block, dishes, channels = visibility.shape[1:]
    tiles = lax.axis_size("tile")
    grps = lax.axis_size("grp")
    f32, bf16, i32 = jnp.float32, jnp.bfloat16, jnp.int32
    groups = len(GROUPS)
    dma = pltpu.SemaphoreType.DMA
    return pl.pallas_call(
        kernel,
        out_shape=(
            jax.ShapeDtypeStruct((2, LEVELS * TRI_LVL), f32),
            jax.ShapeDtypeStruct((2, channels), f32),
        ),
        in_specs=[pl.BlockSpec(memory_space=pltpu.HBM)] * 3,
        out_specs=(pl.BlockSpec(memory_space=pltpu.VMEM), pl.BlockSpec(memory_space=pltpu.VMEM)),
        scratch_shapes=[
            pltpu.VMEM((2, block, dishes, channels), bf16),
            pltpu.VMEM((block, dishes), i32),
            pltpu.VMEM((3, LEVELS * TRI_LVL), i32),
            pltpu.VMEM((block, dishes, channels), bf16),
            pltpu.VMEM((block * dishes, 2, channels), f32),
            pltpu.VMEM((LEVELS, 1, TRI_LVL), i32),
            pltpu.VMEM((LEVELS, 1, TRI_LVL), i32),
            pltpu.VMEM((1, LEVELS * TRI_LVL), i32),
            pltpu.SMEM((1, TRI_LVL), i32),
            pltpu.SMEM((1, TRI_LVL), i32),
            pltpu.SMEM((1, LEVELS * TRI_LVL), i32),
            pltpu.VMEM((block * block, 2 * channels), bf16),
            pltpu.VMEM((2 * CHUNK, channels), f32),
            pltpu.VMEM((2 * CHUNK, channels), f32),
            pltpu.VMEM((PIECES, 2, CHUNK, channels), f32),
            pltpu.VMEM((PIECES, 2, CHUNK, channels), bf16),
            pltpu.VMEM((PIECES, 2, CHUNK, channels), bf16),
            pltpu.VMEM((2, 2 * CHUNK, 2 * channels), bf16),
            pltpu.VMEM((4, channels), f32),
            pltpu.VMEM((tiles, 4, channels), f32),
            [pltpu.VMEM((count, 2 * CHUNK), f32) for _, count in GROUPS],
            [pltpu.VMEM((grps, count, 2 * CHUNK), f32) for _, count in GROUPS],
            pltpu.SemaphoreType.REGULAR((3,)),
            dma((2,)), dma((block,)), dma((3,)),
            dma((LEVELS,)), dma((LEVELS,)),
            dma((PIECES,)), dma((PIECES,)),
            dma((groups, grps - 1)), dma((groups, grps - 1)),
            dma((tiles - 1,)), dma((tiles - 1,)),
        ],
        compiler_params=pltpu.CompilerParams(
            collective_id=0, has_side_effects=True, vmem_limit_bytes=67043328 - 24 * 1024
        ),
        name="closure",
    )(visibility, dish_pair_okay, triangles)


def body(visibility, dish_pair_okay, triangles):
    means, closure = fused(visibility, dish_pair_okay, triangles)
    tile = lax.axis_index("tile")
    width = closure.shape[1] // lax.axis_size("tile")
    return means, lax.dynamic_slice(closure, (0, tile * width), (2, width))


def solution(mesh):
    placed = (P(None, "tile", None, "grp"), P("tile", None), P(None, "tile"))
    return jax.shard_map(
        body,
        mesh=mesh,
        in_specs=placed,
        out_specs=(P(None, "tile"), P(None, ("grp", "tile"))),
        check_vma=False,
    )
```

```python
import jax
import jax.numpy as jnp
from jax import lax
from jax.experimental import pallas as pl
from jax.experimental.pallas import tpu as pltpu
from jax.sharding import PartitionSpec as P

RADIO_BANDS = 1024
TRI_LVL = 1024
LEVELS = 2
CHUNK = 128
CHUNKS = TRI_LVL // CHUNK
PIECES = LEVELS * CHUNKS
UNROLL = 32
ROWS = 4
MESH = pl.DeviceIdType.MESH
NEAR = ((1, 0, 0, 0), (-1, 0, 0, 0), (0, 1, 0, 0), (0, -1, 0, 0), (0, 0, 1, 0), (0, 0, -1, 0), (0, 0, 0, 1))
SECOND = ((0, 0, 0, 1), (2, 0, 0, 0), (0, 2, 0, 0), (0, 0, 2, 0), (0, 0, -2, 0))
THIRD = ((0, 0, 2, 0), (0, 0, -2, 0))
GROUPS = ((0, 8), (8, 4), (12, 2), (14, 1), (15, 1))


def kernel(
    vis_hbm, okay_hbm, tri_hbm, means_ref, closure_ref,
    vis, okay, tri, mask, table, ask, own_pr, s_asked0, s_asked1, s_pr,
    pairs, edge_ab, edge_bc, edge_ac, give, got, split, spec, spec_in, part, arrived,
    known, load_sem, vis_sem, smem_sem, ask_send, ask_recv, row_send, row_recv,
    mean_send, mean_recv, spec_send, spec_recv,
):
    f32, bf16 = jnp.float32, jnp.bfloat16
    tile = lax.axis_index("tile")
    grp = lax.axis_index("grp")
    tiles = lax.axis_size("tile")
    grps = lax.axis_size("grp")
    block, dishes, channels = vis.shape[1:]
    s_asked = (s_asked0, s_asked1)

    load_tri = pltpu.make_async_copy(tri_hbm, tri, load_sem.at[0])
    load_tri.start()
    load_okay = pltpu.make_async_copy(okay_hbm, okay, load_sem.at[1])
    load_okay.start()

    def load_rows(k):
        rows = pl.ds(k * ROWS, ROWS)
        return pltpu.make_async_copy(vis_hbm.at[:, rows], vis.at[:, rows], vis_sem.at[k])

    barrier = pltpu.get_barrier_semaphore()
    spots = (lax.rem(grp, 4), lax.rem(lax.div(tile, 2), 4), lax.div(grp, 4) * 4 + lax.div(tile, 8), lax.rem(tile, 2))

    def tell(sem, steps):
        for step in steps:
            x, y, z, core = (lax.rem(at + d + n, n) for at, d, n in zip(spots, step, (4, 4, 8, 2)))
            there = {"grp": lax.div(z, 4) * 4 + x, "tile": lax.rem(z, 4) * 8 + y * 2 + core}
            pl.semaphore_signal(sem, inc=1, device_id=there, device_id_type=MESH)

    tell(barrier, NEAR)
    partner = [tile + 1 - 2 * lax.rem(tile, 2), tile + 2 - 4 * lax.rem(lax.div(tile, 2), 2)]

    with jax.named_scope("tri_wait"):
        load_tri.wait()
    for k in range(block // ROWS):
        load_rows(k).start()
    first = jnp.bitwise_and(tri[0:1, :], block - 1)
    second = jnp.bitwise_and(tri[1:2, :], block - 1)
    third = tri[2:3, :]
    wanted = second * dishes + third
    for lvl in range(LEVELS):
        ask[lvl] = wanted[:, lvl * TRI_LVL : (lvl + 1) * TRI_LVL]

    with jax.named_scope("barrier"):
        pl.semaphore_wait(barrier, len(NEAR))
    tell(known.at[0], NEAR)
    asks = []
    for lvl in range(LEVELS):
        asks.append(
            pltpu.make_async_remote_copy(
                src_ref=ask.at[lvl], dst_ref=s_asked[lvl],
                send_sem=ask_send.at[lvl], recv_sem=ask_recv.at[lvl],
                device_id={"tile": partner[lvl]}, device_id_type=MESH,
            )
        )
    asks[1].start()
    asks[0].start()
    own_pr[...] = first * dishes + third
    to_pr = pltpu.make_async_copy(own_pr, s_pr, smem_sem)
    to_pr.start()
    pair = (first * block + second).astype(f32)

    with jax.named_scope("flags"):
        load_okay.wait()
        flags_t = jnp.transpose(okay[...].astype(f32)).astype(bf16)
        for c in range(0, block, 2):
            row = lax.broadcasted_iota(jnp.int32, (block, 2 * channels), 0)
            col = lax.broadcasted_iota(jnp.int32, (block, 2 * channels), 1)
            pick = jnp.where(row == c + (col >= channels).astype(jnp.int32), 1.0, 0.0).astype(bf16)
            both = jnp.dot(flags_t, pick, preferred_element_type=f32).astype(bf16)
            mask[c] = both[:, :channels]
            mask[c + 1] = both[:, channels:]

    flat = table.reshape(2 * block * dishes, channels)

    def build(p, _):
        for r in range(0, dishes, 16):
            keep = mask[p, r : r + 16, :]
            base = p * (2 * dishes) + 2 * r
            flat[pl.ds(base, 16, stride=2), :] = (vis[0, p, r : r + 16, :] * keep).astype(f32)
            flat[pl.ds(base + 1, 16, stride=2), :] = (vis[1, p, r : r + 16, :] * keep).astype(f32)
        return 0

    with jax.named_scope("build"):
        for k in range(block // ROWS):
            load_rows(k).wait()
            lax.fori_loop(k * ROWS, (k + 1) * ROWS, build, 0)
    with jax.named_scope("ask_wait"):
        asks[1].wait_recv()

    def gather(index, start, count, dst):
        def body(g, _):
            for u in range(UNROLL):
                j = g * UNROLL + u
                dst[pl.ds(pl.multiple_of(2 * j, 2), 2), :] = table[index[0, start + j]]
            return 0

        lax.fori_loop(0, count // UNROLL, body, 0)

    def serve(lvl, chunk):
        piece = lvl * CHUNKS + chunk
        gather(s_asked[lvl], chunk * CHUNK, CHUNK, edge_bc)
        for r in range(0, CHUNK, 16):
            give[piece, 0, r : r + 16, :] = edge_bc[pl.ds(2 * r, 16, stride=2), :].astype(bf16)
            give[piece, 1, r : r + 16, :] = edge_bc[pl.ds(2 * r + 1, 16, stride=2), :].astype(bf16)
        send = pltpu.make_async_remote_copy(
            src_ref=give.at[piece], dst_ref=got.at[piece],
            send_sem=row_send.at[lvl], recv_sem=row_recv.at[chunk if lvl else CHUNKS],
            device_id={"tile": partner[lvl]}, device_id_type=MESH,
        )
        send.start()
        return send

    def own(lvl):
        start = pl.multiple_of(partner[lvl] * block, block)
        for p in range(block):
            keep = mask[p, pl.ds(start, block), :]
            at = slice(p * block, (p + 1) * block)
            pairs[at, :channels] = vis[0, p, pl.ds(start, block), :] * keep
            pairs[at, channels:] = vis[1, p, pl.ds(start, block), :] * keep
        codes = [pair[:, (lvl * CHUNKS + c) * CHUNK : (lvl * CHUNKS + c + 1) * CHUNK] for c in range(CHUNKS)]
        codes_t = jnp.transpose(jnp.concatenate(codes, axis=0))
        lane = lax.broadcasted_iota(jnp.int32, (CHUNK, block * block), 1).astype(f32)
        for c in range(CHUNKS):
            hot = jnp.where(lane == codes_t[:, c : c + 1], 1.0, 0.0).astype(bf16)
            edge_ab[lvl, c] = jnp.dot(hot, pairs[...], preferred_element_type=f32)
        gather(s_pr, lvl * TRI_LVL, TRI_LVL, edge_ac.at[lvl])

    def multiply(lvl, chunk, r, sums):
        at = pl.ds(pl.multiple_of(r, 16), 16)
        low = pl.ds(pl.multiple_of(CHUNK + r, 16), 16)
        base = pl.multiple_of(2 * (chunk * CHUNK + r), 32)
        a_re = edge_ab[lvl, chunk, at, :channels]
        a_im = edge_ab[lvl, chunk, at, channels:]
        b_re = edge_ac[lvl, pl.ds(base, 16, stride=2), :]
        b_im = edge_ac[lvl, pl.ds(base + 1, 16, stride=2), :]
        p_re = a_re * b_re + a_im * b_im
        p_im = a_im * b_re - a_re * b_im
        c_re = got[lvl * CHUNKS + chunk, 0, at, :].astype(f32)
        c_im = got[lvl * CHUNKS + chunk, 1, at, :].astype(f32)
        re = p_re * c_re - p_im * c_im
        im = p_re * c_im + p_im * c_re
        mag = jnp.sqrt(re * re + im * im)
        re_hi = re.astype(bf16)
        im_hi = im.astype(bf16)
        split[chunk, at, :channels] = re_hi
        split[chunk, at, channels:] = (re - re_hi.astype(f32)).astype(bf16)
        split[chunk, low, :channels] = im_hi
        split[chunk, low, channels:] = (im - im_hi.astype(f32)).astype(bf16)
        return (
            sums[0] + (re[:8] + re[8:]),
            sums[1] + (im[:8] + im[8:]),
            sums[2] + (mag[:8] + mag[8:]),
        )

    def lanes(chunk, row):
        ones = jnp.where(lax.broadcasted_iota(jnp.int32, (8, 2 * channels), 0) == row, 1.0, 0.0).astype(bf16)
        return lax.dot_general(ones, split[chunk], (((1,), (1,)), ((), ())), preferred_element_type=f32)

    def multiply_chunk(lvl, chunk, sums):
        def body(g, sums):
            for u in range(2):
                sums = multiply(lvl, chunk, g * 32 + u * 16, sums)
            return sums

        return lax.fori_loop(0, CHUNK // 32, body, sums)

    def wait_all(sem, ref):
        pltpu.make_async_copy(ref, ref, sem).wait()

    def share(n, total):
        count = GROUPS[n][1]
        part[n][...] = total[:count]
        arrived[n][0] = total[:count]
        for k in range(1, grps):
            send = pltpu.make_async_remote_copy(
                src_ref=part[n], dst_ref=arrived[n].at[k],
                send_sem=mean_send.at[n], recv_sem=mean_recv.at[n],
                device_id={"grp": lax.rem(grp + k, grps)}, device_id_type=MESH,
            )
            send.start()

    rows = [None] * LEVELS
    with jax.named_scope("serve1"):
        rows[1] = [serve(1, c) for c in range(CHUNKS)]
    with jax.named_scope("known0"):
        pl.semaphore_wait(known.at[0], len(NEAR))
    tell(known.at[1], SECOND)
    asks[0].wait_recv()
    with jax.named_scope("serve0"):
        rows[0] = [serve(0, c) for c in range(CHUNKS)]
    to_pr.wait()
    zero = jnp.zeros((8, channels), f32)
    sums = (zero, zero, zero)
    with jax.named_scope("own0"):
        own(0)
    with jax.named_scope("known1"):
        pl.semaphore_wait(known.at[1], len(SECOND))
    tell(known.at[2], THIRD)
    with jax.named_scope("rows0"):
        wait_all(row_recv.at[CHUNKS], got.at[pl.ds(0, CHUNKS)])
    with jax.named_scope("combine0"):
        sums = lax.fori_loop(0, CHUNKS, lambda c, sums: multiply_chunk(0, c, sums), sums)
        total = lanes(0, 0)
        for c in range(1, CHUNKS):
            total = total + lanes(c, c)
    with jax.named_scope("own1"):
        own(1)
    with jax.named_scope("known2"):
        pl.semaphore_wait(known.at[2], len(THIRD))
    with jax.named_scope("share"):
        share(0, total)
    for n, (start, count) in enumerate(GROUPS[1:], 1):
        total = None
        for k in range(count):
            c = start + k - CHUNKS
            with jax.named_scope("rows1"):
                rows[1][c].wait_recv()
            with jax.named_scope("combine1"):
                sums = multiply_chunk(1, c, sums)
                total = lanes(c, k) if k == 0 else total + lanes(c, k)
        with jax.named_scope("share"):
            share(n, total)

    with jax.named_scope("spec_send"):
        for k in range(3):
            spec[k : k + 1, :] = jnp.sum(sums[k], axis=0, keepdims=True)
        spec[3:4, :] = jnp.zeros((1, channels), f32)
        spec_in[0] = spec[...]
        for k in range(1, tiles):
            send = pltpu.make_async_remote_copy(
                src_ref=spec, dst_ref=spec_in.at[k],
                send_sem=spec_send, recv_sem=spec_recv,
                device_id={"tile": lax.rem(tile + k, tiles)}, device_id_type=MESH,
            )
            send.start()

    for n, (start, count) in enumerate(GROUPS):
        with jax.named_scope(f"finish{n}"):
            wait_all(mean_recv.at[n], arrived[n].at[pl.ds(1, grps - 1)])
            total = arrived[n][grp]
            for s in range(1, grps):
                total = total + arrived[n][lax.rem(grp - s + grps, grps)]
            total = total * (1.0 / RADIO_BANDS)
            for k in range(count):
                at = slice((start + k) * CHUNK, (start + k + 1) * CHUNK)
                means_ref[0:1, at] = total[k : k + 1, :CHUNK]
                means_ref[1:2, at] = total[k : k + 1, CHUNK:]

    with jax.named_scope("spec_wait"):
        wait_all(spec_recv, spec_in.at[pl.ds(1, tiles - 1)])
        total = jnp.sum(spec_in[...], axis=0)
        closure_ref[...] = total[0:2] / (1.0 + total[2:3])

    with jax.named_scope("send_wait"):
        for lvl in range(LEVELS):
            asks[lvl].wait_send()
            wait_all(row_send.at[lvl], give.at[pl.ds(lvl * CHUNKS, CHUNKS)])
        for n in range(len(GROUPS)):
            wait_all(mean_send.at[n], arrived[n].at[pl.ds(1, grps - 1)])
        wait_all(spec_send, spec_in.at[pl.ds(1, tiles - 1)])


def fused(visibility, dish_pair_okay, triangles):
    block, dishes, channels = visibility.shape[1:]
    tiles = lax.axis_size("tile")
    grps = lax.axis_size("grp")
    f32, bf16, i32 = jnp.float32, jnp.bfloat16, jnp.int32
    groups = len(GROUPS)
    dma = pltpu.SemaphoreType.DMA
    return pl.pallas_call(
        kernel,
        out_shape=(
            jax.ShapeDtypeStruct((2, LEVELS * TRI_LVL), f32),
            jax.ShapeDtypeStruct((2, channels), f32),
        ),
        in_specs=[pl.BlockSpec(memory_space=pltpu.HBM)] * 3,
        out_specs=(pl.BlockSpec(memory_space=pltpu.VMEM), pl.BlockSpec(memory_space=pltpu.VMEM)),
        scratch_shapes=[
            pltpu.VMEM((2, block, dishes, channels), bf16),
            pltpu.VMEM((block, dishes), i32),
            pltpu.VMEM((3, LEVELS * TRI_LVL), i32),
            pltpu.VMEM((block, dishes, channels), bf16),
            pltpu.VMEM((block * dishes, 2, channels), f32),
            pltpu.VMEM((LEVELS, 1, TRI_LVL), i32),
            pltpu.VMEM((1, LEVELS * TRI_LVL), i32),
            pltpu.SMEM((1, TRI_LVL), i32),
            pltpu.SMEM((1, TRI_LVL), i32),
            pltpu.SMEM((1, LEVELS * TRI_LVL), i32),
            pltpu.VMEM((block * block, 2 * channels), bf16),
            pltpu.VMEM((LEVELS, CHUNKS, CHUNK, 2 * channels), f32),
            pltpu.VMEM((2 * CHUNK, channels), f32),
            pltpu.VMEM((LEVELS, 2 * TRI_LVL, channels), f32),
            pltpu.VMEM((PIECES, 2, CHUNK, channels), bf16),
            pltpu.VMEM((PIECES, 2, CHUNK, channels), bf16),
            pltpu.VMEM((CHUNKS, 2 * CHUNK, 2 * channels), bf16),
            pltpu.VMEM((4, channels), f32),
            pltpu.VMEM((tiles, 4, channels), f32),
            [pltpu.VMEM((count, 2 * CHUNK), f32) for _, count in GROUPS],
            [pltpu.VMEM((grps, count, 2 * CHUNK), f32) for _, count in GROUPS],
            pltpu.SemaphoreType.REGULAR((3,)),
            dma((2,)), dma((block // ROWS,)), dma,
            dma((LEVELS,)), dma((LEVELS,)),
            dma((LEVELS,)), dma((CHUNKS + 1,)),
            dma((groups,)), dma((groups,)),
            dma, dma,
        ],
        compiler_params=pltpu.CompilerParams(
            collective_id=0, has_side_effects=True, vmem_limit_bytes=48 * 2**20
        ),
        name="closure",
    )(*(pltpu.with_memory_space_constraint(x, pltpu.HBM) for x in (visibility, dish_pair_okay, triangles)))


def body(visibility, dish_pair_okay, triangles):
    means, closure = fused(visibility, dish_pair_okay, triangles)
    tile = lax.axis_index("tile")
    width = closure.shape[1] // lax.axis_size("tile")
    return means, lax.dynamic_slice(closure, (0, tile * width), (2, width))


def solution(mesh):
    placed = (P(None, "tile", None, "grp"), P("tile", None), P(None, "tile"))
    return jax.shard_map(
        body,
        mesh=mesh,
        in_specs=placed,
        out_specs=(P(None, "tile"), P(None, ("grp", "tile"))),
        check_vma=False,
    )
```

```python
import jax
import jax.numpy as jnp
from jax import lax
from jax.experimental import pallas as pl
from jax.experimental.pallas import tpu as pltpu
from jax.sharding import PartitionSpec as P

RADIO_BANDS = 1024
TRI_LVL = 1024
LEVELS = 2
CHUNK = 128
CHUNKS = TRI_LVL // CHUNK
PIECES = LEVELS * CHUNKS
UNROLL = 32
ROWS = 4
MESH = pl.DeviceIdType.MESH
ACROSS = ((1, 0, 0, 0), (-1, 0, 0, 0), (0, 0, 1, 0), (0, 0, -1, 0))
NEAR = ((1, 0, 0, 0), (-1, 0, 0, 0), (0, 1, 0, 0), (0, -1, 0, 0), (0, 0, 1, 0), (0, 0, -1, 0), (0, 0, 0, 1))
SECOND = ((0, 0, 0, 1), (2, 0, 0, 0), (0, 2, 0, 0), (0, 0, 2, 0), (0, 0, -2, 0))
THIRD = ((0, 0, 2, 0), (0, 0, -2, 0))
GROUPS = ((0, 8), (8, 4), (12, 2), (14, 1), (15, 1))


def kernel(
    vis_hbm, okay_hbm, tri_hbm, means_ref, closure_ref,
    vis, okay, tri, mask, table, ask, own_pr, s_asked0, s_asked1, s_pr,
    pairs, edge_ab, edge_bc, edge_ac, give, got, split, spec, spec_in, part, arrived,
    known, load_sem, vis_sem, smem_sem, ask_send, ask_recv, row_send, row_recv,
    mean_send, mean_recv, spec_send, spec_recv,
):
    f32, bf16 = jnp.float32, jnp.bfloat16
    tile = lax.axis_index("tile")
    grp = lax.axis_index("grp")
    tiles = lax.axis_size("tile")
    grps = lax.axis_size("grp")
    block, dishes, channels = vis.shape[1:]
    s_asked = (s_asked0, s_asked1)

    load_tri = pltpu.make_async_copy(tri_hbm, tri, load_sem.at[0])
    load_tri.start()
    load_okay = pltpu.make_async_copy(okay_hbm, okay, load_sem.at[1])
    load_okay.start()

    def load_rows(k):
        rows = pl.ds(k * ROWS, ROWS)
        return pltpu.make_async_copy(vis_hbm.at[:, rows], vis.at[:, rows], vis_sem.at[k])

    barrier = pltpu.get_barrier_semaphore()
    spots = (lax.rem(grp, 4), lax.rem(lax.div(tile, 2), 4), lax.div(grp, 4) * 4 + lax.div(tile, 8), lax.rem(tile, 2))

    def there(step):
        x, y, z, core = (lax.rem(at + d + n, n) for at, d, n in zip(spots, step, (4, 4, 8, 2)))
        return {"grp": lax.div(z, 4) * 4 + x, "tile": lax.rem(z, 4) * 8 + y * 2 + core}, (x, y, z)

    def tell(sem, steps):
        for step in steps:
            pl.semaphore_signal(sem, inc=1, device_id=there(step)[0], device_id_type=MESH)

    odd = lax.rem(spots[1], 2)
    pair_step = (0, 1 - 2 * odd, 0, 0)
    cross_step = (0, 2 * odd - 1, 0, 0)
    across = []
    for step, line in ((ACROSS[0], 0), (ACROSS[1], 0), (ACROSS[2], 2), (ACROSS[3], 2), (cross_step, 1)):
        device, place = there(step)
        across.append((device, place[line] > spots[line]))
    higher = sum(jnp.where(up, 1, 0) for _, up in across)
    tell(barrier, ((0, 0, 0, 1), pair_step))
    for device, up in across:

        @pl.when(up)
        def greet():
            pl.semaphore_signal(barrier, inc=1, device_id=device, device_id_type=MESH)

    partner = [tile + 1 - 2 * lax.rem(tile, 2), tile + 2 - 4 * lax.rem(lax.div(tile, 2), 2)]

    with jax.named_scope("tri_wait"):
        load_tri.wait()
    for k in range(block // ROWS):
        load_rows(k).start()
    first = jnp.bitwise_and(tri[0:1, :], block - 1)
    second = jnp.bitwise_and(tri[1:2, :], block - 1)
    third = tri[2:3, :]
    wanted = second * dishes + third
    for lvl in range(LEVELS):
        ask[lvl] = wanted[:, lvl * TRI_LVL : (lvl + 1) * TRI_LVL]

    with jax.named_scope("barrier"):
        pl.semaphore_wait(barrier, 2 + len(across) - higher)
    for device, up in across:

        @pl.when(jnp.logical_not(up))
        def answer():
            pl.semaphore_signal(known.at[0], inc=1, device_id=device, device_id_type=MESH)

    asks = []
    for lvl in range(LEVELS):
        asks.append(
            pltpu.make_async_remote_copy(
                src_ref=ask.at[lvl], dst_ref=s_asked[lvl],
                send_sem=ask_send.at[lvl], recv_sem=ask_recv.at[lvl],
                device_id={"tile": partner[lvl]}, device_id_type=MESH,
            )
        )
    asks[1].start()
    asks[0].start()
    own_pr[...] = first * dishes + third
    to_pr = pltpu.make_async_copy(own_pr, s_pr, smem_sem)
    to_pr.start()
    pair = (first * block + second).astype(f32)

    with jax.named_scope("flags"):
        load_okay.wait()
        flags_t = jnp.transpose(okay[...].astype(f32)).astype(bf16)
        for c in range(0, block, 2):
            row = lax.broadcasted_iota(jnp.int32, (block, 2 * channels), 0)
            col = lax.broadcasted_iota(jnp.int32, (block, 2 * channels), 1)
            pick = jnp.where(row == c + (col >= channels).astype(jnp.int32), 1.0, 0.0).astype(bf16)
            both = jnp.dot(flags_t, pick, preferred_element_type=f32).astype(bf16)
            mask[c] = both[:, :channels]
            mask[c + 1] = both[:, channels:]

    flat = table.reshape(2 * block * dishes, channels)

    def build(p, _):
        for r in range(0, dishes, 16):
            keep = mask[p, r : r + 16, :]
            base = p * (2 * dishes) + 2 * r
            flat[pl.ds(base, 16, stride=2), :] = (vis[0, p, r : r + 16, :] * keep).astype(f32)
            flat[pl.ds(base + 1, 16, stride=2), :] = (vis[1, p, r : r + 16, :] * keep).astype(f32)
        return 0

    with jax.named_scope("build"):
        for k in range(block // ROWS):
            load_rows(k).wait()
            lax.fori_loop(k * ROWS, (k + 1) * ROWS, build, 0)
    with jax.named_scope("ask_wait"):
        asks[1].wait_recv()

    def gather(index, start, count, dst):
        def body(g, _):
            for u in range(UNROLL):
                j = g * UNROLL + u
                dst[pl.ds(pl.multiple_of(2 * j, 2), 2), :] = table[index[0, start + j]]
            return 0

        lax.fori_loop(0, count // UNROLL, body, 0)

    def serve(lvl, chunk):
        piece = lvl * CHUNKS + chunk
        gather(s_asked[lvl], chunk * CHUNK, CHUNK, edge_bc)
        for r in range(0, CHUNK, 16):
            give[piece, 0, r : r + 16, :] = edge_bc[pl.ds(2 * r, 16, stride=2), :].astype(bf16)
            give[piece, 1, r : r + 16, :] = edge_bc[pl.ds(2 * r + 1, 16, stride=2), :].astype(bf16)
        send = pltpu.make_async_remote_copy(
            src_ref=give.at[piece], dst_ref=got.at[piece],
            send_sem=row_send.at[lvl], recv_sem=row_recv.at[chunk if lvl else CHUNKS],
            device_id={"tile": partner[lvl]}, device_id_type=MESH,
        )
        send.start()
        return send

    def own(lvl):
        start = pl.multiple_of(partner[lvl] * block, block)
        for p in range(block):
            keep = mask[p, pl.ds(start, block), :]
            at = slice(p * block, (p + 1) * block)
            pairs[at, :channels] = vis[0, p, pl.ds(start, block), :] * keep
            pairs[at, channels:] = vis[1, p, pl.ds(start, block), :] * keep
        codes = [pair[:, (lvl * CHUNKS + c) * CHUNK : (lvl * CHUNKS + c + 1) * CHUNK] for c in range(CHUNKS)]
        codes_t = jnp.transpose(jnp.concatenate(codes, axis=0))
        lane = lax.broadcasted_iota(jnp.int32, (CHUNK, block * block), 1).astype(f32)
        for c in range(CHUNKS):
            hot = jnp.where(lane == codes_t[:, c : c + 1], 1.0, 0.0).astype(bf16)
            edge_ab[lvl, c] = jnp.dot(hot, pairs[...], preferred_element_type=f32)
        gather(s_pr, lvl * TRI_LVL, TRI_LVL, edge_ac.at[lvl])

    def multiply(lvl, chunk, r, sums):
        at = pl.ds(pl.multiple_of(r, 16), 16)
        low = pl.ds(pl.multiple_of(CHUNK + r, 16), 16)
        base = pl.multiple_of(2 * (chunk * CHUNK + r), 32)
        a_re = edge_ab[lvl, chunk, at, :channels]
        a_im = edge_ab[lvl, chunk, at, channels:]
        b_re = edge_ac[lvl, pl.ds(base, 16, stride=2), :]
        b_im = edge_ac[lvl, pl.ds(base + 1, 16, stride=2), :]
        p_re = a_re * b_re + a_im * b_im
        p_im = a_im * b_re - a_re * b_im
        c_re = got[lvl * CHUNKS + chunk, 0, at, :].astype(f32)
        c_im = got[lvl * CHUNKS + chunk, 1, at, :].astype(f32)
        re = p_re * c_re - p_im * c_im
        im = p_re * c_im + p_im * c_re
        mag = jnp.sqrt(re * re + im * im)
        re_hi = re.astype(bf16)
        im_hi = im.astype(bf16)
        split[chunk, at, :channels] = re_hi
        split[chunk, at, channels:] = (re - re_hi.astype(f32)).astype(bf16)
        split[chunk, low, :channels] = im_hi
        split[chunk, low, channels:] = (im - im_hi.astype(f32)).astype(bf16)
        return (
            sums[0] + (re[:8] + re[8:]),
            sums[1] + (im[:8] + im[8:]),
            sums[2] + (mag[:8] + mag[8:]),
        )

    def lanes(chunk, row):
        ones = jnp.where(lax.broadcasted_iota(jnp.int32, (8, 2 * channels), 0) == row, 1.0, 0.0).astype(bf16)
        return lax.dot_general(ones, split[chunk], (((1,), (1,)), ((), ())), preferred_element_type=f32)

    def multiply_chunk(lvl, chunk, sums):
        def body(g, sums):
            for u in range(2):
                sums = multiply(lvl, chunk, g * 32 + u * 16, sums)
            return sums

        return lax.fori_loop(0, CHUNK // 32, body, sums)

    def wait_all(sem, ref):
        pltpu.make_async_copy(ref, ref, sem).wait()

    def share(n, total):
        count = GROUPS[n][1]
        part[n][...] = total[:count]
        arrived[n][0] = total[:count]
        for k in range(1, grps):
            send = pltpu.make_async_remote_copy(
                src_ref=part[n], dst_ref=arrived[n].at[k],
                send_sem=mean_send.at[n], recv_sem=mean_recv.at[n],
                device_id={"grp": lax.rem(grp + k, grps)}, device_id_type=MESH,
            )
            send.start()

    rows = [None] * LEVELS
    with jax.named_scope("serve1"):
        rows[1] = [serve(1, c) for c in range(CHUNKS)]
    asks[0].wait_recv()
    with jax.named_scope("serve0"):
        rows[0] = [serve(0, c) for c in range(CHUNKS)]
    with jax.named_scope("known0"):

        @pl.when(higher > 0)
        def answered():
            pl.semaphore_wait(known.at[0], higher)

    tell(known.at[1], NEAR)
    to_pr.wait()
    zero = jnp.zeros((8, channels), f32)
    sums = (zero, zero, zero)
    with jax.named_scope("own0"):
        own(0)
    with jax.named_scope("known1"):
        pl.semaphore_wait(known.at[1], len(NEAR))
    tell(known.at[2], SECOND)
    with jax.named_scope("rows0"):
        wait_all(row_recv.at[CHUNKS], got.at[pl.ds(0, CHUNKS)])
    with jax.named_scope("combine0"):
        sums = lax.fori_loop(0, CHUNKS, lambda c, sums: multiply_chunk(0, c, sums), sums)
        total = lanes(0, 0)
        for c in range(1, CHUNKS):
            total = total + lanes(c, c)
    with jax.named_scope("known2"):
        pl.semaphore_wait(known.at[2], len(SECOND))
    tell(known.at[3], THIRD)
    with jax.named_scope("own1"):
        own(1)
    with jax.named_scope("known3"):
        pl.semaphore_wait(known.at[3], len(THIRD))
    with jax.named_scope("share"):
        share(0, total)
    for n, (start, count) in enumerate(GROUPS[1:], 1):
        total = None
        for k in range(count):
            c = start + k - CHUNKS
            with jax.named_scope("rows1"):
                rows[1][c].wait_recv()
            with jax.named_scope("combine1"):
                sums = multiply_chunk(1, c, sums)
                total = lanes(c, k) if k == 0 else total + lanes(c, k)
        with jax.named_scope("share"):
            share(n, total)

    with jax.named_scope("spec_send"):
        width = channels // tiles
        row = lax.broadcasted_iota(jnp.int32, (tiles, channels), 0)
        lane = lax.broadcasted_iota(jnp.int32, (tiles, channels), 1)
        mine = jnp.logical_and(lane >= row * width, lane < (row + 1) * width)
        packed = [jnp.where(mine, jnp.sum(x, axis=0, keepdims=True), 0.0) for x in sums]
        packed = packed[0] + pltpu.roll(packed[1], channels // 4, 1) + pltpu.roll(packed[2], channels // 2, 1)
        spec.reshape(tiles, channels)[...] = packed
        spec_in[0] = spec[tile]
        for k in range(1, tiles):
            send = pltpu.make_async_remote_copy(
                src_ref=spec.at[lax.rem(tile + k, tiles)], dst_ref=spec_in.at[k],
                send_sem=spec_send, recv_sem=spec_recv,
                device_id={"tile": lax.rem(tile + k, tiles)}, device_id_type=MESH,
            )
            send.start()

    for n, (start, count) in enumerate(GROUPS):
        with jax.named_scope(f"finish{n}"):
            wait_all(mean_recv.at[n], arrived[n].at[pl.ds(1, grps - 1)])
            total = arrived[n][grp]
            for s in range(1, grps):
                total = total + arrived[n][lax.rem(grp - s + grps, grps)]
            total = total * (1.0 / RADIO_BANDS)
            for k in range(count):
                at = slice((start + k) * CHUNK, (start + k + 1) * CHUNK)
                means_ref[0:1, at] = total[k : k + 1, :CHUNK]
                means_ref[1:2, at] = total[k : k + 1, CHUNK:]

    with jax.named_scope("spec_wait"):
        wait_all(spec_recv, spec_in.at[pl.ds(1, tiles - 1)])
        total = jnp.sum(spec_in[...], axis=0)
        norm = 1.0 + pltpu.roll(total, channels // 2, 1)
        closure_ref[0:1] = total / norm
        closure_ref[1:2] = pltpu.roll(total, channels - channels // 4, 1) / norm

    with jax.named_scope("send_wait"):
        for lvl in range(LEVELS):
            asks[lvl].wait_send()
            wait_all(row_send.at[lvl], give.at[pl.ds(lvl * CHUNKS, CHUNKS)])
        for n in range(len(GROUPS)):
            wait_all(mean_send.at[n], arrived[n].at[pl.ds(1, grps - 1)])
        wait_all(spec_send, spec_in.at[pl.ds(1, tiles - 1)])


def fused(visibility, dish_pair_okay, triangles):
    block, dishes, channels = visibility.shape[1:]
    tiles = lax.axis_size("tile")
    grps = lax.axis_size("grp")
    f32, bf16, i32 = jnp.float32, jnp.bfloat16, jnp.int32
    groups = len(GROUPS)
    dma = pltpu.SemaphoreType.DMA
    return pl.pallas_call(
        kernel,
        out_shape=(
            jax.ShapeDtypeStruct((2, LEVELS * TRI_LVL), f32),
            jax.ShapeDtypeStruct((2, channels), f32),
        ),
        in_specs=[pl.BlockSpec(memory_space=pltpu.HBM)] * 3,
        out_specs=(pl.BlockSpec(memory_space=pltpu.VMEM), pl.BlockSpec(memory_space=pltpu.VMEM)),
        scratch_shapes=[
            pltpu.VMEM((2, block, dishes, channels), bf16),
            pltpu.VMEM((block, dishes), i32),
            pltpu.VMEM((3, LEVELS * TRI_LVL), i32),
            pltpu.VMEM((block, dishes, channels), bf16),
            pltpu.VMEM((block * dishes, 2, channels), f32),
            pltpu.VMEM((LEVELS, 1, TRI_LVL), i32),
            pltpu.VMEM((1, LEVELS * TRI_LVL), i32),
            pltpu.SMEM((1, TRI_LVL), i32),
            pltpu.SMEM((1, TRI_LVL), i32),
            pltpu.SMEM((1, LEVELS * TRI_LVL), i32),
            pltpu.VMEM((block * block, 2 * channels), bf16),
            pltpu.VMEM((LEVELS, CHUNKS, CHUNK, 2 * channels), f32),
            pltpu.VMEM((2 * CHUNK, channels), f32),
            pltpu.VMEM((LEVELS, 2 * TRI_LVL, channels), f32),
            pltpu.VMEM((PIECES, 2, CHUNK, channels), bf16),
            pltpu.VMEM((PIECES, 2, CHUNK, channels), bf16),
            pltpu.VMEM((CHUNKS, 2 * CHUNK, 2 * channels), bf16),
            pltpu.VMEM((tiles, 1, channels), f32),
            pltpu.VMEM((tiles, 1, channels), f32),
            [pltpu.VMEM((count, 2 * CHUNK), f32) for _, count in GROUPS],
            [pltpu.VMEM((grps, count, 2 * CHUNK), f32) for _, count in GROUPS],
            pltpu.SemaphoreType.REGULAR((4,)),
            dma((2,)), dma((block // ROWS,)), dma,
            dma((LEVELS,)), dma((LEVELS,)),
            dma((LEVELS,)), dma((CHUNKS + 1,)),
            dma((groups,)), dma((groups,)),
            dma, dma,
        ],
        compiler_params=pltpu.CompilerParams(
            collective_id=0, has_side_effects=True, vmem_limit_bytes=48 * 2**20
        ),
        name="closure",
    )(*(pltpu.with_memory_space_constraint(x, pltpu.HBM) for x in (visibility, dish_pair_okay, triangles)))


def body(visibility, dish_pair_okay, triangles):
    means, closure = fused(visibility, dish_pair_okay, triangles)
    tile = lax.axis_index("tile")
    width = closure.shape[1] // lax.axis_size("tile")
    return means, lax.dynamic_slice(closure, (0, tile * width), (2, width))


def solution(mesh):
    placed = (P(None, "tile", None, "grp"), P("tile", None), P(None, "tile"))
    return jax.shard_map(
        body,
        mesh=mesh,
        in_specs=placed,
        out_specs=(P(None, "tile"), P(None, ("grp", "tile"))),
        check_vma=False,
    )
```

```python
import jax
import jax.numpy as jnp
from jax import lax
from jax.experimental import pallas as pl
from jax.experimental.pallas import tpu as pltpu
from jax.sharding import PartitionSpec as P

RADIO_BANDS = 1024
TRI_LVL = 1024
LEVELS = 2
CHUNK = 128
CHUNKS = TRI_LVL // CHUNK
PIECES = LEVELS * CHUNKS
UNROLL = 32
ROWS = 4
MESH = pl.DeviceIdType.MESH
ACROSS = ((1, 0, 0, 0), (-1, 0, 0, 0), (0, 0, 1, 0), (0, 0, -1, 0))
NEAR = ((1, 0, 0, 0), (-1, 0, 0, 0), (0, 1, 0, 0), (0, -1, 0, 0), (0, 0, 1, 0), (0, 0, -1, 0), (0, 0, 0, 1))
SECOND = ((0, 0, 0, 1), (2, 0, 0, 0), (0, 2, 0, 0), (0, 0, 2, 0), (0, 0, -2, 0))
THIRD = ((0, 0, 2, 0), (0, 0, -2, 0))
GROUPS = ((0, 8), (8, 4), (12, 2), (14, 1), (15, 1))


def kernel(
    vis_hbm, okay_hbm, tri_hbm, means_ref, closure_ref,
    vis, okay, tri, mask, table, ask, own_pr, s_asked0, s_asked1, s_pr,
    pairs, edge_ab, edge_bc, edge_ac, give, got, split, spec, spec_in, part, arrived,
    known, load_sem, vis_sem, smem_sem, ask_send, ask_recv, row_send, row_recv,
    mean_send, mean_recv, spec_send, spec_recv,
):
    f32, bf16 = jnp.float32, jnp.bfloat16
    tile = lax.axis_index("tile")
    grp = lax.axis_index("grp")
    tiles = lax.axis_size("tile")
    grps = lax.axis_size("grp")
    block, dishes, channels = vis.shape[1:]
    s_asked = (s_asked0, s_asked1)

    load_tri = pltpu.make_async_copy(tri_hbm, tri, load_sem.at[0])
    load_tri.start()
    load_okay = pltpu.make_async_copy(okay_hbm, okay, load_sem.at[1])
    load_okay.start()

    def load_rows(k):
        rows = pl.ds(k * ROWS, ROWS)
        return pltpu.make_async_copy(vis_hbm.at[:, rows], vis.at[:, rows], vis_sem.at[k])

    barrier = pltpu.get_barrier_semaphore()
    spots = (lax.rem(grp, 4), lax.rem(lax.div(tile, 2), 4), lax.div(grp, 4) * 4 + lax.div(tile, 8), lax.rem(tile, 2))

    def there(step):
        x, y, z, core = (lax.rem(at + d + n, n) for at, d, n in zip(spots, step, (4, 4, 8, 2)))
        return {"grp": lax.div(z, 4) * 4 + x, "tile": lax.rem(z, 4) * 8 + y * 2 + core}, (x, y, z)

    def tell(sem, steps):
        for step in steps:
            pl.semaphore_signal(sem, inc=1, device_id=there(step)[0], device_id_type=MESH)

    odd = lax.rem(spots[1], 2)
    pair_step = (0, 1 - 2 * odd, 0, 0)
    cross_step = (0, 2 * odd - 1, 0, 0)
    across = []
    for step, line in ((ACROSS[0], 0), (ACROSS[1], 0), (ACROSS[2], 2), (ACROSS[3], 2), (cross_step, 1)):
        device, place = there(step)
        across.append((device, place[line] > spots[line]))
    higher = sum(jnp.where(up, 1, 0) for _, up in across)
    tell(barrier, ((0, 0, 0, 1), pair_step))
    for device, up in across:

        @pl.when(up)
        def greet():
            pl.semaphore_signal(barrier, inc=1, device_id=device, device_id_type=MESH)

    partner = [tile + 1 - 2 * lax.rem(tile, 2), tile + 2 - 4 * lax.rem(lax.div(tile, 2), 2)]

    for k in range(block // ROWS):
        load_rows(k).start()
    with jax.named_scope("tri_wait"):
        load_tri.wait()
    first = jnp.bitwise_and(tri[0:1, :], block - 1)
    second = jnp.bitwise_and(tri[1:2, :], block - 1)
    third = tri[2:3, :]
    wanted = second * dishes + third
    for lvl in range(LEVELS):
        ask[lvl] = wanted[:, lvl * TRI_LVL : (lvl + 1) * TRI_LVL]

    with jax.named_scope("barrier"):
        pl.semaphore_wait(barrier, 2 + len(across) - higher)
    for device, up in across:

        @pl.when(jnp.logical_not(up))
        def answer():
            pl.semaphore_signal(known.at[0], inc=1, device_id=device, device_id_type=MESH)

    asks = []
    for lvl in range(LEVELS):
        asks.append(
            pltpu.make_async_remote_copy(
                src_ref=ask.at[lvl], dst_ref=s_asked[lvl],
                send_sem=ask_send.at[lvl], recv_sem=ask_recv.at[lvl],
                device_id={"tile": partner[lvl]}, device_id_type=MESH,
            )
        )
    asks[1].start()
    asks[0].start()
    own_pr[...] = first * dishes + third
    to_pr = pltpu.make_async_copy(own_pr, s_pr, smem_sem)
    to_pr.start()
    pair = (first * block + second).astype(f32)

    with jax.named_scope("flags"):
        load_okay.wait()
        flags_t = jnp.transpose(okay[...].astype(f32)).astype(bf16)
        for c in range(0, block, 2):
            row = lax.broadcasted_iota(jnp.int32, (block, 2 * channels), 0)
            col = lax.broadcasted_iota(jnp.int32, (block, 2 * channels), 1)
            pick = jnp.where(row == c + (col >= channels).astype(jnp.int32), 1.0, 0.0).astype(bf16)
            both = jnp.dot(flags_t, pick, preferred_element_type=f32).astype(bf16)
            mask[c] = both[:, :channels]
            mask[c + 1] = both[:, channels:]

    flat = table.reshape(2 * block * dishes, channels)

    def build(p, _):
        for r in range(0, dishes, 16):
            keep = mask[p, r : r + 16, :]
            base = p * (2 * dishes) + 2 * r
            flat[pl.ds(base, 16, stride=2), :] = (vis[0, p, r : r + 16, :] * keep).astype(f32)
            flat[pl.ds(base + 1, 16, stride=2), :] = (vis[1, p, r : r + 16, :] * keep).astype(f32)
        return 0

    with jax.named_scope("build"):
        for k in range(block // ROWS):
            load_rows(k).wait()
            lax.fori_loop(k * ROWS, (k + 1) * ROWS, build, 0)
    with jax.named_scope("ask_wait"):
        asks[1].wait_recv()

    def gather(index, start, count, dst):
        def body(g, _):
            for u in range(UNROLL):
                j = g * UNROLL + u
                dst[pl.ds(pl.multiple_of(2 * j, 2), 2), :] = table[index[0, start + j]]
            return 0

        lax.fori_loop(0, count // UNROLL, body, 0)

    def serve(lvl, chunk):
        piece = lvl * CHUNKS + chunk
        gather(s_asked[lvl], chunk * CHUNK, CHUNK, edge_bc)
        for r in range(0, CHUNK, 16):
            give[piece, 0, r : r + 16, :] = edge_bc[pl.ds(2 * r, 16, stride=2), :].astype(bf16)
            give[piece, 1, r : r + 16, :] = edge_bc[pl.ds(2 * r + 1, 16, stride=2), :].astype(bf16)
        send = pltpu.make_async_remote_copy(
            src_ref=give.at[piece], dst_ref=got.at[piece],
            send_sem=row_send.at[lvl], recv_sem=row_recv.at[chunk if lvl else CHUNKS],
            device_id={"tile": partner[lvl]}, device_id_type=MESH,
        )
        send.start()
        return send

    def own(lvl):
        start = pl.multiple_of(partner[lvl] * block, block)
        for p in range(block):
            keep = mask[p, pl.ds(start, block), :]
            at = slice(p * block, (p + 1) * block)
            pairs[at, :channels] = vis[0, p, pl.ds(start, block), :] * keep
            pairs[at, channels:] = vis[1, p, pl.ds(start, block), :] * keep
        codes = [pair[:, (lvl * CHUNKS + c) * CHUNK : (lvl * CHUNKS + c + 1) * CHUNK] for c in range(CHUNKS)]
        codes_t = jnp.transpose(jnp.concatenate(codes, axis=0))
        lane = lax.broadcasted_iota(jnp.int32, (CHUNK, block * block), 1).astype(f32)
        for c in range(CHUNKS):
            hot = jnp.where(lane == codes_t[:, c : c + 1], 1.0, 0.0).astype(bf16)
            edge_ab[lvl, c] = jnp.dot(hot, pairs[...], preferred_element_type=f32)
        gather(s_pr, lvl * TRI_LVL, TRI_LVL, edge_ac.at[lvl])

    def multiply(lvl, chunk, r, sums):
        at = pl.ds(pl.multiple_of(r, 16), 16)
        low = pl.ds(pl.multiple_of(CHUNK + r, 16), 16)
        base = pl.multiple_of(2 * (chunk * CHUNK + r), 32)
        a_re = edge_ab[lvl, chunk, at, :channels]
        a_im = edge_ab[lvl, chunk, at, channels:]
        b_re = edge_ac[lvl, pl.ds(base, 16, stride=2), :]
        b_im = edge_ac[lvl, pl.ds(base + 1, 16, stride=2), :]
        p_re = a_re * b_re + a_im * b_im
        p_im = a_im * b_re - a_re * b_im
        c_re = got[lvl * CHUNKS + chunk, 0, at, :].astype(f32)
        c_im = got[lvl * CHUNKS + chunk, 1, at, :].astype(f32)
        re = p_re * c_re - p_im * c_im
        im = p_re * c_im + p_im * c_re
        mag = jnp.sqrt(re * re + im * im)
        re_hi = re.astype(bf16)
        im_hi = im.astype(bf16)
        split[chunk, at, :channels] = re_hi
        split[chunk, at, channels:] = (re - re_hi.astype(f32)).astype(bf16)
        split[chunk, low, :channels] = im_hi
        split[chunk, low, channels:] = (im - im_hi.astype(f32)).astype(bf16)
        return (
            sums[0] + (re[:8] + re[8:]),
            sums[1] + (im[:8] + im[8:]),
            sums[2] + (mag[:8] + mag[8:]),
        )

    def lanes(chunk, row):
        ones = jnp.where(lax.broadcasted_iota(jnp.int32, (8, 2 * channels), 0) == row, 1.0, 0.0).astype(bf16)
        return lax.dot_general(ones, split[chunk], (((1,), (1,)), ((), ())), preferred_element_type=f32)

    def multiply_chunk(lvl, chunk, sums):
        def body(g, sums):
            for u in range(2):
                sums = multiply(lvl, chunk, g * 32 + u * 16, sums)
            return sums

        return lax.fori_loop(0, CHUNK // 32, body, sums)

    def wait_all(sem, ref):
        pltpu.make_async_copy(ref, ref, sem).wait()

    def share(n, total):
        count = GROUPS[n][1]
        part[n][...] = total[:count]
        arrived[n][0] = total[:count]
        for k in range(1, grps):
            send = pltpu.make_async_remote_copy(
                src_ref=part[n], dst_ref=arrived[n].at[k],
                send_sem=mean_send.at[n], recv_sem=mean_recv.at[n],
                device_id={"grp": lax.rem(grp + k, grps)}, device_id_type=MESH,
            )
            send.start()

    rows = [None] * LEVELS
    with jax.named_scope("serve1"):
        rows[1] = [serve(1, c) for c in range(CHUNKS)]
    asks[0].wait_recv()
    with jax.named_scope("serve0"):
        rows[0] = [serve(0, c) for c in range(CHUNKS)]
    with jax.named_scope("known0"):

        @pl.when(higher > 0)
        def answered():
            pl.semaphore_wait(known.at[0], higher)

    tell(known.at[1], NEAR)
    to_pr.wait()
    zero = jnp.zeros((8, channels), f32)
    sums = (zero, zero, zero)
    with jax.named_scope("own0"):
        own(0)
    with jax.named_scope("known1"):
        pl.semaphore_wait(known.at[1], len(NEAR))
    tell(known.at[2], SECOND)
    with jax.named_scope("rows0"):
        wait_all(row_recv.at[CHUNKS], got.at[pl.ds(0, CHUNKS)])
    with jax.named_scope("combine0"):
        sums = lax.fori_loop(0, CHUNKS, lambda c, sums: multiply_chunk(0, c, sums), sums)
        total = lanes(0, 0)
        for c in range(1, CHUNKS):
            total = total + lanes(c, c)
    with jax.named_scope("known2"):
        pl.semaphore_wait(known.at[2], len(SECOND))
    tell(known.at[3], THIRD)
    with jax.named_scope("own1"):
        own(1)
    with jax.named_scope("known3"):
        pl.semaphore_wait(known.at[3], len(THIRD))
    with jax.named_scope("share"):
        share(0, total)
    for n, (start, count) in enumerate(GROUPS[1:], 1):
        total = None
        for k in range(count):
            c = start + k - CHUNKS
            with jax.named_scope("rows1"):
                rows[1][c].wait_recv()
            with jax.named_scope("combine1"):
                sums = multiply_chunk(1, c, sums)
                total = lanes(c, k) if k == 0 else total + lanes(c, k)
        with jax.named_scope("share"):
            share(n, total)

    with jax.named_scope("spec_send"):
        width = channels // tiles
        row = lax.broadcasted_iota(jnp.int32, (tiles, channels), 0)
        lane = lax.broadcasted_iota(jnp.int32, (tiles, channels), 1)
        mine = jnp.logical_and(lane >= row * width, lane < (row + 1) * width)
        packed = [jnp.where(mine, jnp.sum(x, axis=0, keepdims=True), 0.0) for x in sums]
        packed = packed[0] + pltpu.roll(packed[1], channels // 4, 1) + pltpu.roll(packed[2], channels // 2, 1)
        spec.reshape(tiles, channels)[...] = packed
        spec_in[0] = spec[tile]
        for k in range(1, tiles):
            send = pltpu.make_async_remote_copy(
                src_ref=spec.at[lax.rem(tile + k, tiles)], dst_ref=spec_in.at[k],
                send_sem=spec_send, recv_sem=spec_recv,
                device_id={"tile": lax.rem(tile + k, tiles)}, device_id_type=MESH,
            )
            send.start()

    for n, (start, count) in enumerate(GROUPS):
        with jax.named_scope(f"finish{n}"):
            wait_all(mean_recv.at[n], arrived[n].at[pl.ds(1, grps - 1)])
            total = arrived[n][grp]
            for s in range(1, grps):
                total = total + arrived[n][lax.rem(grp - s + grps, grps)]
            total = total * (1.0 / RADIO_BANDS)
            for k in range(count):
                at = slice((start + k) * CHUNK, (start + k + 1) * CHUNK)
                means_ref[0:1, at] = total[k : k + 1, :CHUNK]
                means_ref[1:2, at] = total[k : k + 1, CHUNK:]

    with jax.named_scope("spec_wait"):
        wait_all(spec_recv, spec_in.at[pl.ds(1, tiles - 1)])
        total = jnp.sum(spec_in[...], axis=0)
        norm = 1.0 + pltpu.roll(total, channels // 2, 1)
        closure_ref[0:1] = total / norm
        closure_ref[1:2] = pltpu.roll(total, channels - channels // 4, 1) / norm

    with jax.named_scope("send_wait"):
        for lvl in range(LEVELS):
            asks[lvl].wait_send()
            wait_all(row_send.at[lvl], give.at[pl.ds(lvl * CHUNKS, CHUNKS)])
        for n in range(len(GROUPS)):
            wait_all(mean_send.at[n], arrived[n].at[pl.ds(1, grps - 1)])
        wait_all(spec_send, spec_in.at[pl.ds(1, tiles - 1)])


def fused(visibility, dish_pair_okay, triangles):
    block, dishes, channels = visibility.shape[1:]
    tiles = lax.axis_size("tile")
    grps = lax.axis_size("grp")
    f32, bf16, i32 = jnp.float32, jnp.bfloat16, jnp.int32
    groups = len(GROUPS)
    dma = pltpu.SemaphoreType.DMA
    return pl.pallas_call(
        kernel,
        out_shape=(
            jax.ShapeDtypeStruct((2, LEVELS * TRI_LVL), f32),
            jax.ShapeDtypeStruct((2, channels), f32),
        ),
        in_specs=[pl.BlockSpec(memory_space=pltpu.HBM)] * 3,
        out_specs=(pl.BlockSpec(memory_space=pltpu.VMEM), pl.BlockSpec(memory_space=pltpu.VMEM)),
        scratch_shapes=[
            pltpu.VMEM((2, block, dishes, channels), bf16),
            pltpu.VMEM((block, dishes), i32),
            pltpu.VMEM((3, LEVELS * TRI_LVL), i32),
            pltpu.VMEM((block, dishes, channels), bf16),
            pltpu.VMEM((block * dishes, 2, channels), f32),
            pltpu.VMEM((LEVELS, 1, TRI_LVL), i32),
            pltpu.VMEM((1, LEVELS * TRI_LVL), i32),
            pltpu.SMEM((1, TRI_LVL), i32),
            pltpu.SMEM((1, TRI_LVL), i32),
            pltpu.SMEM((1, LEVELS * TRI_LVL), i32),
            pltpu.VMEM((block * block, 2 * channels), bf16),
            pltpu.VMEM((LEVELS, CHUNKS, CHUNK, 2 * channels), f32),
            pltpu.VMEM((2 * CHUNK, channels), f32),
            pltpu.VMEM((LEVELS, 2 * TRI_LVL, channels), f32),
            pltpu.VMEM((PIECES, 2, CHUNK, channels), bf16),
            pltpu.VMEM((PIECES, 2, CHUNK, channels), bf16),
            pltpu.VMEM((CHUNKS, 2 * CHUNK, 2 * channels), bf16),
            pltpu.VMEM((tiles, 1, channels), f32),
            pltpu.VMEM((tiles, 1, channels), f32),
            [pltpu.VMEM((count, 2 * CHUNK), f32) for _, count in GROUPS],
            [pltpu.VMEM((grps, count, 2 * CHUNK), f32) for _, count in GROUPS],
            pltpu.SemaphoreType.REGULAR((4,)),
            dma((2,)), dma((block // ROWS,)), dma,
            dma((LEVELS,)), dma((LEVELS,)),
            dma((LEVELS,)), dma((CHUNKS + 1,)),
            dma((groups,)), dma((groups,)),
            dma, dma,
        ],
        compiler_params=pltpu.CompilerParams(
            collective_id=0, has_side_effects=True, vmem_limit_bytes=48 * 2**20
        ),
        name="closure",
    )(*(pltpu.with_memory_space_constraint(x, pltpu.HBM) for x in (visibility, dish_pair_okay, triangles)))


def body(visibility, dish_pair_okay, triangles):
    means, closure = fused(visibility, dish_pair_okay, triangles)
    tile = lax.axis_index("tile")
    width = closure.shape[1] // lax.axis_size("tile")
    return means, lax.dynamic_slice(closure, (0, tile * width), (2, width))


def solution(mesh):
    placed = (P(None, "tile", None, "grp"), P("tile", None), P(None, "tile"))
    return jax.shard_map(
        body,
        mesh=mesh,
        in_specs=placed,
        out_specs=(P(None, "tile"), P(None, ("grp", "tile"))),
        check_vma=False,
    )
```

```python
import jax
import jax.numpy as jnp
from jax import lax
from jax.experimental import pallas as pl
from jax.experimental.pallas import tpu as pltpu
from jax.sharding import PartitionSpec as P

RADIO_BANDS = 1024
TRI_LVL = 1024
LEVELS = 2
CHUNK = 128
CHUNKS = TRI_LVL // CHUNK
PIECES = LEVELS * CHUNKS
UNROLL = 32
ROWS = 4
MESH = pl.DeviceIdType.MESH
ACROSS = ((1, 0, 0, 0), (-1, 0, 0, 0), (0, 0, 1, 0), (0, 0, -1, 0))
NEAR = ((1, 0, 0, 0), (-1, 0, 0, 0), (0, 1, 0, 0), (0, -1, 0, 0), (0, 0, 1, 0), (0, 0, -1, 0), (0, 0, 0, 1))
SECOND = ((0, 0, 0, 1), (2, 0, 0, 0), (0, 2, 0, 0), (0, 0, 2, 0), (0, 0, -2, 0))
THIRD = ((0, 0, 2, 0), (0, 0, -2, 0))
GROUPS = ((0, 8), (8, 4), (12, 2), (14, 1), (15, 1))


def kernel(
    vis_hbm, okay_hbm, tri_hbm, means_ref, closure_ref,
    vis, okay, tri, mask, table, ask, own_pr, s_asked0, s_asked1, s_pr,
    pairs, edge_ab, edge_bc, edge_ac, give, got, split, spec, spec_in, part, arrived,
    known, load_sem, vis_sem, smem_sem, ask_send, ask_recv, row_send, row_recv,
    mean_send, mean_recv, spec_send, spec_recv,
):
    f32, bf16 = jnp.float32, jnp.bfloat16
    tile = lax.axis_index("tile")
    grp = lax.axis_index("grp")
    tiles = lax.axis_size("tile")
    grps = lax.axis_size("grp")
    block, dishes, channels = vis.shape[1:]
    s_asked = (s_asked0, s_asked1)

    load_tri = pltpu.make_async_copy(tri_hbm, tri, load_sem.at[0])
    load_tri.start()
    load_okay = pltpu.make_async_copy(okay_hbm, okay, load_sem.at[1])
    load_okay.start()

    def load_rows(k):
        rows = pl.ds(k * ROWS, ROWS)
        return pltpu.make_async_copy(vis_hbm.at[:, rows], vis.at[:, rows], vis_sem.at[k])

    barrier = pltpu.get_barrier_semaphore()
    spots = (lax.rem(grp, 4), lax.rem(lax.div(tile, 2), 4), lax.div(grp, 4) * 4 + lax.div(tile, 8), lax.rem(tile, 2))

    def there(step):
        x, y, z, core = (lax.rem(at + d + n, n) for at, d, n in zip(spots, step, (4, 4, 8, 2)))
        return {"grp": lax.div(z, 4) * 4 + x, "tile": lax.rem(z, 4) * 8 + y * 2 + core}, (x, y, z)

    def tell(sem, steps):
        for step in steps:
            pl.semaphore_signal(sem, inc=1, device_id=there(step)[0], device_id_type=MESH)

    odd = lax.rem(spots[1], 2)
    pair_step = (0, 1 - 2 * odd, 0, 0)
    cross_step = (0, 2 * odd - 1, 0, 0)
    across = []
    for step, line in ((ACROSS[0], 0), (ACROSS[1], 0), (ACROSS[2], 2), (ACROSS[3], 2), (cross_step, 1)):
        device, place = there(step)
        across.append((device, place[line] > spots[line]))
    higher = sum(jnp.where(up, 1, 0) for _, up in across)
    tell(barrier, ((0, 0, 0, 1), pair_step))
    for device, up in across:

        @pl.when(up)
        def greet():
            pl.semaphore_signal(barrier, inc=1, device_id=device, device_id_type=MESH)

    partner = [tile + 1 - 2 * lax.rem(tile, 2), tile + 2 - 4 * lax.rem(lax.div(tile, 2), 2)]

    for k in range(block // ROWS):
        load_rows(k).start()
    with jax.named_scope("tri_wait"):
        load_tri.wait()
    first = jnp.bitwise_and(tri[0:1, :], block - 1)
    second = jnp.bitwise_and(tri[1:2, :], block - 1)
    third = tri[2:3, :]
    wanted = second * dishes + third
    for lvl in range(LEVELS):
        ask[lvl] = wanted[:, lvl * TRI_LVL : (lvl + 1) * TRI_LVL]

    with jax.named_scope("okay"):
        load_okay.wait()
        flags_t = jnp.transpose(okay[...].astype(f32)).astype(bf16)
    with jax.named_scope("barrier"):
        pl.semaphore_wait(barrier, 2 + len(across) - higher)
    for device, up in across:

        @pl.when(jnp.logical_not(up))
        def answer():
            pl.semaphore_signal(known.at[0], inc=1, device_id=device, device_id_type=MESH)

    asks = []
    for lvl in range(LEVELS):
        asks.append(
            pltpu.make_async_remote_copy(
                src_ref=ask.at[lvl], dst_ref=s_asked[lvl],
                send_sem=ask_send.at[lvl], recv_sem=ask_recv.at[lvl],
                device_id={"tile": partner[lvl]}, device_id_type=MESH,
            )
        )
    asks[1].start()
    asks[0].start()

    with jax.named_scope("flags"):
        for c in range(0, block, 2):
            row = lax.broadcasted_iota(jnp.int32, (block, 2 * channels), 0)
            col = lax.broadcasted_iota(jnp.int32, (block, 2 * channels), 1)
            pick = jnp.where(row == c + (col >= channels).astype(jnp.int32), 1.0, 0.0).astype(bf16)
            both = jnp.dot(flags_t, pick, preferred_element_type=f32).astype(bf16)
            mask[c] = both[:, :channels]
            mask[c + 1] = both[:, channels:]

    flat = table.reshape(2 * block * dishes, channels)

    def build(p, _):
        for r in range(0, dishes, 16):
            keep = mask[p, r : r + 16, :]
            base = p * (2 * dishes) + 2 * r
            flat[pl.ds(base, 16, stride=2), :] = (vis[0, p, r : r + 16, :] * keep).astype(f32)
            flat[pl.ds(base + 1, 16, stride=2), :] = (vis[1, p, r : r + 16, :] * keep).astype(f32)
        return 0

    with jax.named_scope("build"):
        for k in range(block // ROWS):
            load_rows(k).wait()
            lax.fori_loop(k * ROWS, (k + 1) * ROWS, build, 0)
    own_pr[...] = first * dishes + third
    to_pr = pltpu.make_async_copy(own_pr, s_pr, smem_sem)
    to_pr.start()
    pair = (first * block + second).astype(f32)
    with jax.named_scope("ask_wait"):
        asks[1].wait_recv()

    def gather(index, start, count, dst):
        def body(g, _):
            for u in range(UNROLL):
                j = g * UNROLL + u
                dst[pl.ds(pl.multiple_of(2 * j, 2), 2), :] = table[index[0, start + j]]
            return 0

        lax.fori_loop(0, count // UNROLL, body, 0)

    def serve(lvl, chunk):
        piece = lvl * CHUNKS + chunk
        gather(s_asked[lvl], chunk * CHUNK, CHUNK, edge_bc)
        for r in range(0, CHUNK, 16):
            give[piece, 0, r : r + 16, :] = edge_bc[pl.ds(2 * r, 16, stride=2), :].astype(bf16)
            give[piece, 1, r : r + 16, :] = edge_bc[pl.ds(2 * r + 1, 16, stride=2), :].astype(bf16)
        send = pltpu.make_async_remote_copy(
            src_ref=give.at[piece], dst_ref=got.at[piece],
            send_sem=row_send.at[lvl], recv_sem=row_recv.at[chunk if lvl else CHUNKS],
            device_id={"tile": partner[lvl]}, device_id_type=MESH,
        )
        send.start()
        return send

    def own(lvl):
        start = pl.multiple_of(partner[lvl] * block, block)
        for p in range(block):
            keep = mask[p, pl.ds(start, block), :]
            at = slice(p * block, (p + 1) * block)
            pairs[at, :channels] = vis[0, p, pl.ds(start, block), :] * keep
            pairs[at, channels:] = vis[1, p, pl.ds(start, block), :] * keep
        codes = [pair[:, (lvl * CHUNKS + c) * CHUNK : (lvl * CHUNKS + c + 1) * CHUNK] for c in range(CHUNKS)]
        codes_t = jnp.transpose(jnp.concatenate(codes, axis=0))
        lane = lax.broadcasted_iota(jnp.int32, (CHUNK, block * block), 1).astype(f32)
        for c in range(CHUNKS):
            hot = jnp.where(lane == codes_t[:, c : c + 1], 1.0, 0.0).astype(bf16)
            edge_ab[lvl, c] = jnp.dot(hot, pairs[...], preferred_element_type=f32)
        gather(s_pr, lvl * TRI_LVL, TRI_LVL, edge_ac.at[lvl])

    def multiply(lvl, chunk, r, sums):
        at = pl.ds(pl.multiple_of(r, 16), 16)
        low = pl.ds(pl.multiple_of(CHUNK + r, 16), 16)
        base = pl.multiple_of(2 * (chunk * CHUNK + r), 32)
        a_re = edge_ab[lvl, chunk, at, :channels]
        a_im = edge_ab[lvl, chunk, at, channels:]
        b_re = edge_ac[lvl, pl.ds(base, 16, stride=2), :]
        b_im = edge_ac[lvl, pl.ds(base + 1, 16, stride=2), :]
        p_re = a_re * b_re + a_im * b_im
        p_im = a_im * b_re - a_re * b_im
        c_re = got[lvl * CHUNKS + chunk, 0, at, :].astype(f32)
        c_im = got[lvl * CHUNKS + chunk, 1, at, :].astype(f32)
        re = p_re * c_re - p_im * c_im
        im = p_re * c_im + p_im * c_re
        mag = jnp.sqrt(re * re + im * im)
        re_hi = re.astype(bf16)
        im_hi = im.astype(bf16)
        split[chunk, at, :channels] = re_hi
        split[chunk, at, channels:] = (re - re_hi.astype(f32)).astype(bf16)
        split[chunk, low, :channels] = im_hi
        split[chunk, low, channels:] = (im - im_hi.astype(f32)).astype(bf16)
        return (
            sums[0] + (re[:8] + re[8:]),
            sums[1] + (im[:8] + im[8:]),
            sums[2] + (mag[:8] + mag[8:]),
        )

    def lanes(chunk, row):
        ones = jnp.where(lax.broadcasted_iota(jnp.int32, (8, 2 * channels), 0) == row, 1.0, 0.0).astype(bf16)
        return lax.dot_general(ones, split[chunk], (((1,), (1,)), ((), ())), preferred_element_type=f32)

    def multiply_chunk(lvl, chunk, sums):
        def body(g, sums):
            for u in range(2):
                sums = multiply(lvl, chunk, g * 32 + u * 16, sums)
            return sums

        return lax.fori_loop(0, CHUNK // 32, body, sums)

    def wait_all(sem, ref):
        pltpu.make_async_copy(ref, ref, sem).wait()

    def share(n, total):
        count = GROUPS[n][1]
        part[n][...] = total[:count]
        arrived[n][0] = total[:count]
        for k in range(1, grps):
            send = pltpu.make_async_remote_copy(
                src_ref=part[n], dst_ref=arrived[n].at[k],
                send_sem=mean_send.at[n], recv_sem=mean_recv.at[n],
                device_id={"grp": lax.rem(grp + k, grps)}, device_id_type=MESH,
            )
            send.start()

    half = lax.div(spots[2], 4)

    def relay(turn, stage):
        @pl.when(turn == 1)
        def pass_on():
            if stage == 0:

                @pl.when(higher > 0)
                def answered():
                    pl.semaphore_wait(known.at[0], higher)

                tell(known.at[1], NEAR)
            elif stage == 1:
                pl.semaphore_wait(known.at[1], len(NEAR))
                tell(known.at[2], SECOND)
            else:
                pl.semaphore_wait(known.at[2], len(SECOND))
                tell(known.at[3], THIRD)

    rows = [None] * LEVELS
    with jax.named_scope("serve1"):
        rows[1] = [serve(1, c) for c in range(CHUNKS)]
    relay(half, 0)
    asks[0].wait_recv()
    with jax.named_scope("serve0"):
        rows[0] = [serve(0, c) for c in range(CHUNKS)]
    relay(half, 1)
    to_pr.wait()
    zero = jnp.zeros((8, channels), f32)
    sums = (zero, zero, zero)
    with jax.named_scope("own0"):
        own(0)
    relay(half, 2)
    relay(1 - half, 0)
    with jax.named_scope("rows0"):
        wait_all(row_recv.at[CHUNKS], got.at[pl.ds(0, CHUNKS)])
    with jax.named_scope("combine0"):
        sums = lax.fori_loop(0, CHUNKS, lambda c, sums: multiply_chunk(0, c, sums), sums)
        total = lanes(0, 0)
        for c in range(1, CHUNKS):
            total = total + lanes(c, c)
    relay(1 - half, 1)
    with jax.named_scope("own1"):
        own(1)
    relay(1 - half, 2)
    with jax.named_scope("known3"):
        pl.semaphore_wait(known.at[3], len(THIRD))
    with jax.named_scope("share"):
        share(0, total)
    for n, (start, count) in enumerate(GROUPS[1:], 1):
        total = None
        for k in range(count):
            c = start + k - CHUNKS
            with jax.named_scope("rows1"):
                rows[1][c].wait_recv()
            with jax.named_scope("combine1"):
                sums = multiply_chunk(1, c, sums)
                total = lanes(c, k) if k == 0 else total + lanes(c, k)
        with jax.named_scope("share"):
            share(n, total)

    with jax.named_scope("spec_send"):
        width = channels // tiles
        row = lax.broadcasted_iota(jnp.int32, (tiles, channels), 0)
        lane = lax.broadcasted_iota(jnp.int32, (tiles, channels), 1)
        mine = jnp.logical_and(lane >= row * width, lane < (row + 1) * width)
        packed = [jnp.where(mine, jnp.sum(x, axis=0, keepdims=True), 0.0) for x in sums]
        packed = packed[0] + pltpu.roll(packed[1], channels // 4, 1) + pltpu.roll(packed[2], channels // 2, 1)
        spec.reshape(tiles, channels)[...] = packed
        spec_in[0] = spec[tile]
        for k in range(1, tiles):
            send = pltpu.make_async_remote_copy(
                src_ref=spec.at[lax.rem(tile + k, tiles)], dst_ref=spec_in.at[k],
                send_sem=spec_send, recv_sem=spec_recv,
                device_id={"tile": lax.rem(tile + k, tiles)}, device_id_type=MESH,
            )
            send.start()

    for n, (start, count) in enumerate(GROUPS):
        with jax.named_scope(f"finish{n}"):
            wait_all(mean_recv.at[n], arrived[n].at[pl.ds(1, grps - 1)])
            total = arrived[n][grp]
            for s in range(1, grps):
                total = total + arrived[n][lax.rem(grp - s + grps, grps)]
            total = total * (1.0 / RADIO_BANDS)
            for k in range(count):
                at = slice((start + k) * CHUNK, (start + k + 1) * CHUNK)
                means_ref[0:1, at] = total[k : k + 1, :CHUNK]
                means_ref[1:2, at] = total[k : k + 1, CHUNK:]

    with jax.named_scope("spec_wait"):
        wait_all(spec_recv, spec_in.at[pl.ds(1, tiles - 1)])
        total = jnp.sum(spec_in[...], axis=0)
        norm = 1.0 + pltpu.roll(total, channels // 2, 1)
        closure_ref[0:1] = total / norm
        closure_ref[1:2] = pltpu.roll(total, channels - channels // 4, 1) / norm

    with jax.named_scope("send_wait"):
        for lvl in range(LEVELS):
            asks[lvl].wait_send()
            wait_all(row_send.at[lvl], give.at[pl.ds(lvl * CHUNKS, CHUNKS)])
        for n in range(len(GROUPS)):
            wait_all(mean_send.at[n], arrived[n].at[pl.ds(1, grps - 1)])
        wait_all(spec_send, spec_in.at[pl.ds(1, tiles - 1)])


def fused(visibility, dish_pair_okay, triangles):
    block, dishes, channels = visibility.shape[1:]
    tiles = lax.axis_size("tile")
    grps = lax.axis_size("grp")
    f32, bf16, i32 = jnp.float32, jnp.bfloat16, jnp.int32
    groups = len(GROUPS)
    dma = pltpu.SemaphoreType.DMA
    return pl.pallas_call(
        kernel,
        out_shape=(
            jax.ShapeDtypeStruct((2, LEVELS * TRI_LVL), f32),
            jax.ShapeDtypeStruct((2, channels), f32),
        ),
        in_specs=[pl.BlockSpec(memory_space=pltpu.HBM)] * 3,
        out_specs=(pl.BlockSpec(memory_space=pltpu.VMEM), pl.BlockSpec(memory_space=pltpu.VMEM)),
        scratch_shapes=[
            pltpu.VMEM((2, block, dishes, channels), bf16),
            pltpu.VMEM((block, dishes), i32),
            pltpu.VMEM((3, LEVELS * TRI_LVL), i32),
            pltpu.VMEM((block, dishes, channels), bf16),
            pltpu.VMEM((block * dishes, 2, channels), f32),
            pltpu.VMEM((LEVELS, 1, TRI_LVL), i32),
            pltpu.VMEM((1, LEVELS * TRI_LVL), i32),
            pltpu.SMEM((1, TRI_LVL), i32),
            pltpu.SMEM((1, TRI_LVL), i32),
            pltpu.SMEM((1, LEVELS * TRI_LVL), i32),
            pltpu.VMEM((block * block, 2 * channels), bf16),
            pltpu.VMEM((LEVELS, CHUNKS, CHUNK, 2 * channels), f32),
            pltpu.VMEM((2 * CHUNK, channels), f32),
            pltpu.VMEM((LEVELS, 2 * TRI_LVL, channels), f32),
            pltpu.VMEM((PIECES, 2, CHUNK, channels), bf16),
            pltpu.VMEM((PIECES, 2, CHUNK, channels), bf16),
            pltpu.VMEM((CHUNKS, 2 * CHUNK, 2 * channels), bf16),
            pltpu.VMEM((tiles, 1, channels), f32),
            pltpu.VMEM((tiles, 1, channels), f32),
            [pltpu.VMEM((count, 2 * CHUNK), f32) for _, count in GROUPS],
            [pltpu.VMEM((grps, count, 2 * CHUNK), f32) for _, count in GROUPS],
            pltpu.SemaphoreType.REGULAR((4,)),
            dma((2,)), dma((block // ROWS,)), dma,
            dma((LEVELS,)), dma((LEVELS,)),
            dma((LEVELS,)), dma((CHUNKS + 1,)),
            dma((groups,)), dma((groups,)),
            dma, dma,
        ],
        compiler_params=pltpu.CompilerParams(
            collective_id=0, has_side_effects=True, vmem_limit_bytes=48 * 2**20
        ),
        name="closure",
    )(*(pltpu.with_memory_space_constraint(x, pltpu.HBM) for x in (visibility, dish_pair_okay, triangles)))


def body(visibility, dish_pair_okay, triangles):
    means, closure = fused(visibility, dish_pair_okay, triangles)
    tile = lax.axis_index("tile")
    width = closure.shape[1] // lax.axis_size("tile")
    return means, lax.dynamic_slice(closure, (0, tile * width), (2, width))


def solution(mesh):
    placed = (P(None, "tile", None, "grp"), P("tile", None), P(None, "tile"))
    return jax.shard_map(
        body,
        mesh=mesh,
        in_specs=placed,
        out_specs=(P(None, "tile"), P(None, ("grp", "tile"))),
        check_vma=False,
    )
```

```python
import jax
import jax.numpy as jnp
from jax import lax
from jax.experimental import pallas as pl
from jax.experimental.pallas import tpu as pltpu
from jax.sharding import PartitionSpec as P

RADIO_BANDS = 1024
TRI_LVL = 1024
LEVELS = 2
CHUNK = 128
CHUNKS = TRI_LVL // CHUNK
PIECES = LEVELS * CHUNKS
UNROLL = 32
ROWS = 4
MESH = pl.DeviceIdType.MESH
ACROSS = ((1, 0, 0, 0), (-1, 0, 0, 0), (0, 0, 1, 0), (0, 0, -1, 0))
NEAR = ((1, 0, 0, 0), (-1, 0, 0, 0), (0, 1, 0, 0), (0, -1, 0, 0), (0, 0, 1, 0), (0, 0, -1, 0), (0, 0, 0, 1))
SECOND = ((0, 0, 0, 1), (2, 0, 0, 0), (0, 2, 0, 0), (0, 0, 2, 0), (0, 0, -2, 0))
THIRD = ((0, 0, 2, 0), (0, 0, -2, 0))
GROUPS = ((0, 8), (8, 4), (12, 2), (14, 1), (15, 1))


def kernel(
    vis_hbm, okay_hbm, tri_hbm, means_ref, closure_ref,
    vis, okay, tri, mask, table, ask, own_pr, s_asked0, s_asked1, s_pr,
    pairs, edge_ab, edge_bc, edge_ac, give, got, split, spec, spec_in, part, arrived,
    known, load_sem, vis_sem, smem_sem, ask_send, ask_recv, row_send, row_recv,
    mean_send, mean_recv, spec_send, spec_recv,
):
    f32, bf16 = jnp.float32, jnp.bfloat16
    tile = lax.axis_index("tile")
    grp = lax.axis_index("grp")
    tiles = lax.axis_size("tile")
    grps = lax.axis_size("grp")
    block, dishes, channels = vis.shape[1:]
    s_asked = (s_asked0, s_asked1)

    load_tri = pltpu.make_async_copy(tri_hbm, tri, load_sem.at[0])
    load_tri.start()
    load_okay = pltpu.make_async_copy(okay_hbm, okay, load_sem.at[1])
    load_okay.start()

    def load_rows(k):
        rows = pl.ds(k * ROWS, ROWS)
        return pltpu.make_async_copy(vis_hbm.at[:, rows], vis.at[:, rows], vis_sem.at[k])

    barrier = pltpu.get_barrier_semaphore()
    spots = (lax.rem(grp, 4), lax.rem(lax.div(tile, 2), 4), lax.div(grp, 4) * 4 + lax.div(tile, 8), lax.rem(tile, 2))

    def there(step):
        x, y, z, core = (lax.rem(at + d + n, n) for at, d, n in zip(spots, step, (4, 4, 8, 2)))
        return {"grp": lax.div(z, 4) * 4 + x, "tile": lax.rem(z, 4) * 8 + y * 2 + core}, (x, y, z)

    def tell(sem, steps):
        for step in steps:
            pl.semaphore_signal(sem, inc=1, device_id=there(step)[0], device_id_type=MESH)

    odd = lax.rem(spots[1], 2)
    pair_step = (0, 1 - 2 * odd, 0, 0)
    cross_step = (0, 2 * odd - 1, 0, 0)
    across = []
    for step, line in ((ACROSS[0], 0), (ACROSS[1], 0), (ACROSS[2], 2), (ACROSS[3], 2), (cross_step, 1)):
        device, place = there(step)
        across.append((device, place[line] > spots[line]))
    higher = sum(jnp.where(up, 1, 0) for _, up in across)
    tell(barrier, ((0, 0, 0, 1), pair_step))
    for device, up in across:

        @pl.when(up)
        def greet():
            pl.semaphore_signal(barrier, inc=1, device_id=device, device_id_type=MESH)

    partner = [tile + 1 - 2 * lax.rem(tile, 2), tile + 2 - 4 * lax.rem(lax.div(tile, 2), 2)]

    for k in range(block // ROWS):
        load_rows(k).start()
    with jax.named_scope("tri_wait"):
        load_tri.wait()
    first = jnp.bitwise_and(tri[0:1, :], block - 1)
    second = jnp.bitwise_and(tri[1:2, :], block - 1)
    third = tri[2:3, :]
    wanted = second * dishes + third
    for lvl in range(LEVELS):
        ask[lvl] = wanted[:, lvl * TRI_LVL : (lvl + 1) * TRI_LVL]

    with jax.named_scope("okay"):
        load_okay.wait()
        flags_t = jnp.transpose(okay[...].astype(f32)).astype(bf16)
    with jax.named_scope("barrier"):
        pl.semaphore_wait(barrier, 2 + len(across) - higher)
    for device, up in across:

        @pl.when(jnp.logical_not(up))
        def answer():
            pl.semaphore_signal(known.at[0], inc=1, device_id=device, device_id_type=MESH)

    asks = []
    for lvl in range(LEVELS):
        asks.append(
            pltpu.make_async_remote_copy(
                src_ref=ask.at[lvl], dst_ref=s_asked[lvl],
                send_sem=ask_send.at[lvl], recv_sem=ask_recv.at[lvl],
                device_id={"tile": partner[lvl]}, device_id_type=MESH,
            )
        )
    asks[1].start()
    asks[0].start()

    with jax.named_scope("flags"):
        for c in range(0, block, 2):
            row = lax.broadcasted_iota(jnp.int32, (block, 2 * channels), 0)
            col = lax.broadcasted_iota(jnp.int32, (block, 2 * channels), 1)
            pick = jnp.where(row == c + (col >= channels).astype(jnp.int32), 1.0, 0.0).astype(bf16)
            both = jnp.dot(flags_t, pick, preferred_element_type=f32).astype(bf16)
            mask[c] = both[:, :channels]
            mask[c + 1] = both[:, channels:]

    flat = table.reshape(2 * block * dishes, channels)

    def build(p, _):
        for r in range(0, dishes, 16):
            keep = mask[p, r : r + 16, :]
            base = p * (2 * dishes) + 2 * r
            flat[pl.ds(base, 16, stride=2), :] = (vis[0, p, r : r + 16, :] * keep).astype(f32)
            flat[pl.ds(base + 1, 16, stride=2), :] = (vis[1, p, r : r + 16, :] * keep).astype(f32)
        return 0

    with jax.named_scope("build"):
        for k in range(block // ROWS):
            load_rows(k).wait()
            lax.fori_loop(k * ROWS, (k + 1) * ROWS, build, 0)
    own_pr[...] = first * dishes + third
    to_pr = pltpu.make_async_copy(own_pr, s_pr, smem_sem)
    to_pr.start()
    pair = (first * block + second).astype(f32)
    with jax.named_scope("ask_wait"):
        asks[1].wait_recv()

    def gather(index, start, count, dst):
        def body(g, _):
            for u in range(UNROLL):
                j = g * UNROLL + u
                dst[pl.ds(pl.multiple_of(2 * j, 2), 2), :] = table[index[0, start + j]]
            return 0

        lax.fori_loop(0, count // UNROLL, body, 0)

    def serve(lvl, chunk):
        piece = lvl * CHUNKS + chunk
        gather(s_asked[lvl], chunk * CHUNK, CHUNK, edge_bc)
        for r in range(0, CHUNK, 16):
            give[piece, 0, r : r + 16, :] = edge_bc[pl.ds(2 * r, 16, stride=2), :].astype(bf16)
            give[piece, 1, r : r + 16, :] = edge_bc[pl.ds(2 * r + 1, 16, stride=2), :].astype(bf16)
        send = pltpu.make_async_remote_copy(
            src_ref=give.at[piece], dst_ref=got.at[piece],
            send_sem=row_send.at[lvl], recv_sem=row_recv.at[chunk if lvl else CHUNKS],
            device_id={"tile": partner[lvl]}, device_id_type=MESH,
        )
        send.start()
        return send

    def own(lvl):
        start = pl.multiple_of(partner[lvl] * block, block)
        for p in range(block):
            keep = mask[p, pl.ds(start, block), :]
            at = slice(p * block, (p + 1) * block)
            pairs[at, :channels] = vis[0, p, pl.ds(start, block), :] * keep
            pairs[at, channels:] = vis[1, p, pl.ds(start, block), :] * keep
        codes = [pair[:, (lvl * CHUNKS + c) * CHUNK : (lvl * CHUNKS + c + 1) * CHUNK] for c in range(CHUNKS)]
        codes_t = jnp.transpose(jnp.concatenate(codes, axis=0))
        lane = lax.broadcasted_iota(jnp.int32, (CHUNK, block * block), 1).astype(f32)
        for c in range(CHUNKS):
            hot = jnp.where(lane == codes_t[:, c : c + 1], 1.0, 0.0).astype(bf16)
            edge_ab[lvl, c] = jnp.dot(hot, pairs[...], preferred_element_type=f32)
        gather(s_pr, lvl * TRI_LVL, TRI_LVL, edge_ac.at[lvl])

    def multiply(lvl, chunk, r, sums):
        at = pl.ds(pl.multiple_of(r, 16), 16)
        low = pl.ds(pl.multiple_of(CHUNK + r, 16), 16)
        base = pl.multiple_of(2 * (chunk * CHUNK + r), 32)
        a_re = edge_ab[lvl, chunk, at, :channels]
        a_im = edge_ab[lvl, chunk, at, channels:]
        b_re = edge_ac[lvl, pl.ds(base, 16, stride=2), :]
        b_im = edge_ac[lvl, pl.ds(base + 1, 16, stride=2), :]
        p_re = a_re * b_re + a_im * b_im
        p_im = a_im * b_re - a_re * b_im
        c_re = got[lvl * CHUNKS + chunk, 0, at, :].astype(f32)
        c_im = got[lvl * CHUNKS + chunk, 1, at, :].astype(f32)
        re = p_re * c_re - p_im * c_im
        im = p_re * c_im + p_im * c_re
        mag = jnp.sqrt(re * re + im * im)
        re_hi = re.astype(bf16)
        im_hi = im.astype(bf16)
        split[chunk, at, :channels] = re_hi
        split[chunk, at, channels:] = (re - re_hi.astype(f32)).astype(bf16)
        split[chunk, low, :channels] = im_hi
        split[chunk, low, channels:] = (im - im_hi.astype(f32)).astype(bf16)
        return (
            sums[0] + (re[:8] + re[8:]),
            sums[1] + (im[:8] + im[8:]),
            sums[2] + (mag[:8] + mag[8:]),
        )

    def lanes(chunk, row):
        ones = jnp.where(lax.broadcasted_iota(jnp.int32, (8, 2 * channels), 0) == row, 1.0, 0.0).astype(bf16)
        return lax.dot_general(ones, split[chunk], (((1,), (1,)), ((), ())), preferred_element_type=f32)

    def multiply_chunk(lvl, chunk, sums):
        def body(g, sums):
            for u in range(2):
                sums = multiply(lvl, chunk, g * 32 + u * 16, sums)
            return sums

        return lax.fori_loop(0, CHUNK // 32, body, sums)

    def wait_all(sem, ref):
        pltpu.make_async_copy(ref, ref, sem).wait()

    def share(n, total):
        count = GROUPS[n][1]
        part[n][...] = total[:count]
        arrived[n][0] = total[:count]
        for k in range(1, grps):
            send = pltpu.make_async_remote_copy(
                src_ref=part[n], dst_ref=arrived[n].at[k],
                send_sem=mean_send.at[n], recv_sem=mean_recv.at[n],
                device_id={"grp": lax.rem(grp + k, grps)}, device_id_type=MESH,
            )
            send.start()

    rows = [None] * LEVELS
    with jax.named_scope("serve1"):
        rows[1] = [serve(1, c) for c in range(CHUNKS)]
    asks[0].wait_recv()
    with jax.named_scope("serve0"):
        rows[0] = [serve(0, c) for c in range(CHUNKS)]
    with jax.named_scope("known0"):

        @pl.when(higher > 0)
        def answered():
            pl.semaphore_wait(known.at[0], higher)

    tell(known.at[1], NEAR)
    to_pr.wait()
    zero = jnp.zeros((8, channels), f32)
    sums = (zero, zero, zero)
    with jax.named_scope("own0"):
        own(0)
    with jax.named_scope("known1"):
        pl.semaphore_wait(known.at[1], len(NEAR))
    tell(known.at[2], SECOND)
    with jax.named_scope("rows0"):
        wait_all(row_recv.at[CHUNKS], got.at[pl.ds(0, CHUNKS)])
    with jax.named_scope("combine0"):
        sums = lax.fori_loop(0, CHUNKS, lambda c, sums: multiply_chunk(0, c, sums), sums)
        total = lanes(0, 0)
        for c in range(1, CHUNKS):
            total = total + lanes(c, c)
    with jax.named_scope("known2"):
        pl.semaphore_wait(known.at[2], len(SECOND))
    tell(known.at[3], THIRD)
    with jax.named_scope("own1"):
        own(1)
    with jax.named_scope("known3"):
        pl.semaphore_wait(known.at[3], len(THIRD))
    with jax.named_scope("share"):
        share(0, total)
    for n, (start, count) in enumerate(GROUPS[1:], 1):
        total = None
        for k in range(count):
            c = start + k - CHUNKS
            with jax.named_scope("rows1"):
                rows[1][c].wait_recv()
            with jax.named_scope("combine1"):
                sums = multiply_chunk(1, c, sums)
                total = lanes(c, k) if k == 0 else total + lanes(c, k)
        with jax.named_scope("share"):
            share(n, total)

    with jax.named_scope("spec_send"):
        width = channels // tiles
        row = lax.broadcasted_iota(jnp.int32, (tiles, channels), 0)
        lane = lax.broadcasted_iota(jnp.int32, (tiles, channels), 1)
        mine = jnp.logical_and(lane >= row * width, lane < (row + 1) * width)
        packed = [jnp.where(mine, jnp.sum(x, axis=0, keepdims=True), 0.0) for x in sums]
        packed = packed[0] + pltpu.roll(packed[1], channels // 4, 1) + pltpu.roll(packed[2], channels // 2, 1)
        spec.reshape(tiles, channels)[...] = packed
        spec_in[0] = spec[tile]
        for k in range(1, tiles):
            send = pltpu.make_async_remote_copy(
                src_ref=spec.at[lax.rem(tile + k, tiles)], dst_ref=spec_in.at[k],
                send_sem=spec_send, recv_sem=spec_recv,
                device_id={"tile": lax.rem(tile + k, tiles)}, device_id_type=MESH,
            )
            send.start()

    for n, (start, count) in enumerate(GROUPS):
        with jax.named_scope(f"finish{n}"):
            wait_all(mean_recv.at[n], arrived[n].at[pl.ds(1, grps - 1)])
            total = arrived[n][grp]
            for s in range(1, grps):
                total = total + arrived[n][lax.rem(grp - s + grps, grps)]
            total = total * (1.0 / RADIO_BANDS)
            for k in range(count):
                at = slice((start + k) * CHUNK, (start + k + 1) * CHUNK)
                means_ref[0:1, at] = total[k : k + 1, :CHUNK]
                means_ref[1:2, at] = total[k : k + 1, CHUNK:]

    with jax.named_scope("spec_wait"):
        wait_all(spec_recv, spec_in.at[pl.ds(1, tiles - 1)])
        total = jnp.sum(spec_in[...], axis=0)
        norm = 1.0 + pltpu.roll(total, channels // 2, 1)
        closure_ref[0:1] = total / norm
        closure_ref[1:2] = pltpu.roll(total, channels - channels // 4, 1) / norm

    with jax.named_scope("send_wait"):
        for lvl in range(LEVELS):
            asks[lvl].wait_send()
            wait_all(row_send.at[lvl], give.at[pl.ds(lvl * CHUNKS, CHUNKS)])
        for n in range(len(GROUPS)):
            wait_all(mean_send.at[n], arrived[n].at[pl.ds(1, grps - 1)])
        wait_all(spec_send, spec_in.at[pl.ds(1, tiles - 1)])


def fused(visibility, dish_pair_okay, triangles):
    block, dishes, channels = visibility.shape[1:]
    tiles = lax.axis_size("tile")
    grps = lax.axis_size("grp")
    f32, bf16, i32 = jnp.float32, jnp.bfloat16, jnp.int32
    groups = len(GROUPS)
    dma = pltpu.SemaphoreType.DMA
    return pl.pallas_call(
        kernel,
        out_shape=(
            jax.ShapeDtypeStruct((2, LEVELS * TRI_LVL), f32),
            jax.ShapeDtypeStruct((2, channels), f32),
        ),
        in_specs=[pl.BlockSpec(memory_space=pltpu.HBM)] * 3,
        out_specs=(pl.BlockSpec(memory_space=pltpu.VMEM), pl.BlockSpec(memory_space=pltpu.VMEM)),
        scratch_shapes=[
            pltpu.VMEM((2, block, dishes, channels), bf16),
            pltpu.VMEM((block, dishes), i32),
            pltpu.VMEM((3, LEVELS * TRI_LVL), i32),
            pltpu.VMEM((block, dishes, channels), bf16),
            pltpu.VMEM((block * dishes, 2, channels), f32),
            pltpu.VMEM((LEVELS, 1, TRI_LVL), i32),
            pltpu.VMEM((1, LEVELS * TRI_LVL), i32),
            pltpu.SMEM((1, TRI_LVL), i32),
            pltpu.SMEM((1, TRI_LVL), i32),
            pltpu.SMEM((1, LEVELS * TRI_LVL), i32),
            pltpu.VMEM((block * block, 2 * channels), bf16),
            pltpu.VMEM((LEVELS, CHUNKS, CHUNK, 2 * channels), f32),
            pltpu.VMEM((2 * CHUNK, channels), f32),
            pltpu.VMEM((LEVELS, 2 * TRI_LVL, channels), f32),
            pltpu.VMEM((PIECES, 2, CHUNK, channels), bf16),
            pltpu.VMEM((PIECES, 2, CHUNK, channels), bf16),
            pltpu.VMEM((CHUNKS, 2 * CHUNK, 2 * channels), bf16),
            pltpu.VMEM((tiles, 1, channels), f32),
            pltpu.VMEM((tiles, 1, channels), f32),
            [pltpu.VMEM((count, 2 * CHUNK), f32) for _, count in GROUPS],
            [pltpu.VMEM((grps, count, 2 * CHUNK), f32) for _, count in GROUPS],
            pltpu.SemaphoreType.REGULAR((4,)),
            dma((2,)), dma((block // ROWS,)), dma,
            dma((LEVELS,)), dma((LEVELS,)),
            dma((LEVELS,)), dma((CHUNKS + 1,)),
            dma((groups,)), dma((groups,)),
            dma, dma,
        ],
        compiler_params=pltpu.CompilerParams(
            collective_id=0, has_side_effects=True, vmem_limit_bytes=48 * 2**20
        ),
        name="closure",
    )(*(pltpu.with_memory_space_constraint(x, pltpu.HBM) for x in (visibility, dish_pair_okay, triangles)))


def body(visibility, dish_pair_okay, triangles):
    means, closure = fused(visibility, dish_pair_okay, triangles)
    tile = lax.axis_index("tile")
    width = closure.shape[1] // lax.axis_size("tile")
    return means, lax.dynamic_slice(closure, (0, tile * width), (2, width))


def solution(mesh):
    placed = (P(None, "tile", None, "grp"), P("tile", None), P(None, "tile"))
    return jax.shard_map(
        body,
        mesh=mesh,
        in_specs=placed,
        out_specs=(P(None, "tile"), P(None, ("grp", "tile"))),
        check_vma=False,
    )
```
